32 devices in a mesh: seq: 16 (over z, y, x), slide: 2 (over core).
Axes of the slice: x: 2, y: 2, z: 4, core: 2. Of those that a mesh axis runs over, the one named last changes fastest.
Arguments:
- tile_embed: bfloat16 [16384, 768], P(('slide', 'seq')), parts along dimension 0, may hold values from -6 to 6
- valid_tiles: int32 [2], P('slide'), parts along dimension 0, may hold values from 4096 to 8192
- offsets: int32 [16], replicated, may hold values from 0 to 15
- norm_gain: float32 [768], replicated, may hold values from 0.1 to 1.9
- w_qkv: bfloat16 [768, 2304], replicated
- sub_gain: float32 [768], replicated, may hold values from 0.1 to 1.9
- w_out: bfloat16 [768, 768], replicated, may hold values from -0.21875 to 0.21875
Outputs:
- encoded: bfloat16 [16384, 768], P(('slide', 'seq')), parts along dimension 0
The draws below stay inside these ranges and needn't reach their ends.
There are 2 independent parts, one for each index of `slide`. The reference program is written for one: setup_inputs(seed, part) draws one part's arguments, and reference() takes and returns one part's arrays. A program takes and returns all parts, laid end to end along the dimension named above; an argument that names none is the same for every part. Nothing has to cross between parts.
All inputs are finite; a program needn't handle non-finite values.
Results may differ from the reference program's by a relative error of at most 0.0078.
Values may be sent and summed in bfloat16 or wider, within the bound.
A program may use at most 128 MiB of HBM per device.

```python
import jax
import jax.numpy as jnp
from jax import lax

D = 768
HEADS = 16
DEVICE_TOKENS = 512
SLIDE_TOKENS = 8192
NEAR_SPAN = 2
MIDDLE_DILATION = 4
FAR_DILATION = 16
MIDDLE_SPAN = 4
FAR_SEGMENT_SPAN = 8
N_SEQ = 16


def draw_w_qkv(key, part):
    key_query = jax.random.fold_in(key, 11)
    key_keys = jax.random.fold_in(key, 12)
    key_values = jax.random.fold_in(key, 13)
    spread_scale = D ** (-0.5)
    query_w = jax.random.normal(key_query, (D, D), jnp.float32) * spread_scale
    value_w = jax.random.normal(key_values, (D, D), jnp.float32) * spread_scale
    key_w = jax.random.normal(key_keys, (D, D), jnp.float32) * spread_scale
    return jnp.concatenate([query_w, key_w, value_w], axis=1).astype(jnp.bfloat16)


def with_ends(entries, key, least, high):
    extent = entries.shape
    spot = [jax.random.randint(jax.random.fold_in(key, axis), (), 0, extent[axis]) for axis in range(len(extent))]
    entries = entries.at[tuple(spot)].set(least)
    longest = extent.index(max(extent))
    spot[longest] = (spot[longest] + 1) % extent[longest]
    return entries.at[tuple(spot)].set(high)


def block_levels(own_key, extent, shards, low, top_value):
    def one(position, parts):
        steps = jax.random.uniform(jax.random.fold_in(jax.random.fold_in(own_key, 6), position), (parts,), jnp.float32, low / len(shards), top_value / len(shards))
        return jnp.repeat(jnp.exp(steps), extent[position] // parts).reshape((-1,) + (1,) * (len(extent) - position - 1))

    loudness = one(*shards[0])
    for cut in shards[1:]:
        loudness = loudness * one(*cut)
    return loudness


def noise(stream_key, dims, spread, bound, shards=(), kind=jnp.bfloat16):
    drawn = jax.random.normal(stream_key, dims, jnp.float32) * spread
    if len(shards) > 0:
        drawn = block_levels(stream_key, dims, shards, -0.22, 0.18) * drawn
    return jnp.clip(drawn, min=-bound, max=bound).astype(kind)


def setup_inputs(seed: int = 0, part: int = 0) -> dict:
    key_list = jax.random.split(jax.random.key(seed), 8)
    own_keys = jax.random.split(jax.random.fold_in(key_list[7], part), 8)
    return {
        "tile_embed": noise(own_keys[0], (SLIDE_TOKENS, D), 1.0, 6.0, ((0, 16),)),
        "valid_tiles": jax.random.randint(own_keys[1], (1,), SLIDE_TOKENS // 2, SLIDE_TOKENS + 1).astype(jnp.int32),
        "offsets": with_ends(jax.random.randint(key_list[2], (HEADS,), 0, 16), jax.random.fold_in(key_list[2], 1), 0, 15).astype(jnp.int32),
        "norm_gain": jnp.clip(1.0 + 0.18 * jax.random.normal(key_list[3], (D,), jnp.float32), 0.1, 1.9),
        "w_qkv": draw_w_qkv(jax.random.fold_in(key_list[7], 71), part),
        "sub_gain": jnp.clip(1.0 + 0.18 * jax.random.normal(key_list[5], (D,), jnp.float32), 0.1, 1.9),
        "w_out": noise(key_list[6], (D, D), D ** -0.5, 0.21875),
    }


NEGATIVE = -1e+30
EPSILON = 1e-05

def layer_norm(matrix, gain_row):
    average = lax.optimization_barrier(jnp.mean(matrix, axis=-1, keepdims=True))
    centred = matrix - average
    variance = lax.optimization_barrier(jnp.mean(centred * centred, axis=-1, keepdims=True))
    return centred * lax.rsqrt(variance + EPSILON) * gain_row

def attend(packed):
    query_rows, key_rows, value_rows, key_alive = packed
    scores = jnp.dot(query_rows, key_rows.T, preferred_element_type=jnp.float32) * query_rows.shape[-1] ** (-0.5)
    scores = jnp.where(key_alive[None, :], scores, NEGATIVE)
    row_max = lax.optimization_barrier(jnp.max(scores, axis=1))
    weights = jnp.where(key_alive[None, :], jnp.exp(scores - row_max[:, None]), 0.0)
    row_sum = lax.optimization_barrier(jnp.sum(weights, axis=1))
    numerator = jnp.dot(weights.astype(jnp.bfloat16), value_rows, preferred_element_type=jnp.float32)
    return (row_max, row_sum, numerator)

def branch(query_rows, key_rows, value_rows, offsets, valid_tile_count, seg_len, dilation):
    head_count, length, head_size = query_rows.shape
    segments = length // seg_len
    per_segment = seg_len // dilation
    chosen_mod = (offsets % dilation).astype(jnp.int32)
    picker = jnp.broadcast_to(chosen_mod[:, None, None, None, None], (head_count, segments, per_segment, 1, head_size))

    def select(matrix):
        tiled = matrix.reshape(head_count, segments, per_segment, dilation, head_size)
        return jnp.take_along_axis(tiled, picker, axis=3)[:, :, :, 0, :].reshape(head_count * segments, per_segment, head_size)
    positions = jnp.arange(segments, dtype=jnp.int32)[None, :, None] * seg_len + jnp.arange(per_segment, dtype=jnp.int32)[None, None, :] * dilation + chosen_mod[:, None, None]
    key_alive = (positions < valid_tile_count).reshape(head_count * segments, per_segment)
    row_max, row_sum, numerator = lax.map(attend, (select(query_rows), select(key_rows), select(value_rows), key_alive))
    onehot = jnp.arange(dilation, dtype=jnp.int32)[None, :] == chosen_mod[:, None]
    row_max = jnp.where(onehot[:, None, None, :], row_max.reshape(head_count, segments, per_segment, 1), NEGATIVE)
    row_sum = jnp.where(onehot[:, None, None, :], row_sum.reshape(head_count, segments, per_segment, 1), 0.0)
    numerator = jnp.where(onehot[:, None, None, :, None], numerator.reshape(head_count, segments, per_segment, 1, head_size), 0.0)
    return (row_max.reshape(head_count, length), row_sum.reshape(head_count, length), numerator.reshape(head_count, length, head_size))

def reference(tile_embed, valid_tiles, offsets, norm_gain, w_qkv, sub_gain, w_out):
    relaid = tile_embed.reshape(N_SEQ, DEVICE_TOKENS, D).transpose(1, 0, 2).reshape(SLIDE_TOKENS, D)
    normed = layer_norm(relaid.astype(jnp.float32), norm_gain).astype(jnp.bfloat16)
    projected = jnp.dot(normed, w_qkv, preferred_element_type=jnp.float32).astype(jnp.bfloat16)
    triple = projected.reshape(SLIDE_TOKENS, 3, HEADS, D // HEADS).transpose(1, 2, 0, 3)
    valid_tile_count = valid_tiles[0]
    exchange_plans = [(NEAR_SPAN * DEVICE_TOKENS, 1), (MIDDLE_SPAN * DEVICE_TOKENS, MIDDLE_DILATION), (FAR_SEGMENT_SPAN * DEVICE_TOKENS, FAR_DILATION), (SLIDE_TOKENS, FAR_DILATION)]
    branch_list = [branch(triple[0], triple[1], triple[2], offsets, valid_tile_count, seg_len, dilation) for seg_len, dilation in exchange_plans]
    highest = branch_list[0][0]
    for result in branch_list[1:]:
        highest = jnp.maximum(highest, result[0])
    denom = jnp.zeros_like(highest)
    numer_all = jnp.zeros_like(branch_list[0][2])
    for result in branch_list:
        factor = jnp.exp(result[0] - highest)
        denom = denom + factor * result[1]
        numer_all = numer_all + factor[:, :, None] * result[2]
    attended = (numer_all / jnp.maximum(denom, 1.0)[:, :, None]).astype(jnp.bfloat16)
    flattened = attended.transpose(1, 0, 2).reshape(SLIDE_TOKENS, D)
    sub_normed = layer_norm(flattened.astype(jnp.float32), sub_gain).astype(jnp.bfloat16)
    return (relaid.astype(jnp.float32) + jnp.dot(sub_normed, w_out, preferred_element_type=jnp.float32)).astype(jnp.bfloat16)
```

```python
import functools

import jax
import jax.numpy as jnp
import numpy as np
from jax import lax
from jax.experimental import pallas as pl
from jax.experimental.pallas import tpu as pltpu
from jax.sharding import PartitionSpec as P

MIDDLE_DILATION = 4
FAR_DILATION = 16
NEGATIVE = -1e30
EPSILON = 1e-05
LOG2E = 1.4426950408889634
AUG = 16
VMEM_LIMIT = 60 * 1024 * 1024


def layer_norm_rows(x, gain):
    average = jnp.mean(x, axis=-1, keepdims=True)
    centred = x - average
    variance = jnp.mean(centred * centred, axis=-1, keepdims=True)
    return centred * lax.rsqrt(variance + EPSILON) * gain


def project_into(dst, x_ref, gain_ref, w_ref, chunk, skip=0):
    normed = layer_norm_rows(x_ref[...].astype(jnp.float32), gain_ref[...]).astype(jnp.bfloat16)

    @pl.loop(0, (w_ref.shape[0] - skip) // chunk)
    def _(i):
        rows = pl.ds(pl.multiple_of(i * chunk, chunk), chunk)
        dst[rows, :] = lax.dot_general(
            w_ref[pl.ds(pl.multiple_of(i * chunk + skip, chunk), chunk), :], normed, (((1,), (1,)), ((), ())), preferred_element_type=jnp.float32
        ).astype(jnp.bfloat16)


def project_kernel(heads, offs, x_ref, gain_ref, w_ref, proj_ref, mid_ref, fark_ref, farv_ref, far_scr):
    rows, width = x_ref.shape
    size = width // heads
    lanes = rows // MIDDLE_DILATION
    few = rows // FAR_DILATION
    project_into(proj_ref, x_ref, gain_ref, w_ref, 256)
    src = lax.broadcasted_iota(jnp.int32, (lanes, lanes), 0)
    dst = lax.broadcasted_iota(jnp.int32, (lanes, lanes), 1)
    for head in range(heads):
        phase = offs[head] % FAR_DILATION
        quarter = phase % MIDDLE_DILATION
        shift = (phase // MIDDLE_DILATION) * few
        pick = ((src == dst + shift) & (dst < few)).astype(jnp.bfloat16)
        for part in range(2):
            base = part * width + head * size
            block = proj_ref[
                width + base : width + base + size,
                pl.ds(pl.multiple_of(quarter * lanes, lanes), lanes),
            ]
            mid_ref[base : base + size, :] = block
            far_scr[base : base + size, :] = jnp.dot(
                block, pick, preferred_element_type=jnp.float32
            )
    fark_ref[...] = far_scr[:width, :].T[:few].astype(jnp.bfloat16)
    farv_ref[...] = far_scr[width:, :].T[:few].astype(jnp.bfloat16)


def aug_rows(first, lanes, second=None):
    spot = lax.broadcasted_iota(jnp.int32, (AUG, lanes), 0)
    rows = jnp.where(spot == 0, first, 0.0)
    if second is not None:
        rows = jnp.where(spot == 1, second, rows)
    return rows.astype(jnp.bfloat16)


def weighted_values(value, weight):
    scaled = (value.astype(jnp.float32) * weight).astype(jnp.bfloat16)
    return jnp.concatenate([scaled, aug_rows(weight, value.shape[1])], axis=0)


def scores_of(keys, queries):
    return lax.dot_general(
        keys, queries, (((0,), (0,)), ((), ())), preferred_element_type=jnp.float32
    )


def own_kernel(scale, per_step, size, valid, q_ref, k_ref, v_ref, pos_ref, out_ref):
    lanes = q_ref.shape[1]
    alive = pos_ref[...] + lax.axis_index("seq") * lanes < valid[0]
    bias = aug_rows(jnp.where(alive, 0.0, NEGATIVE), lanes)
    weight = jnp.where(alive, 1.0, 0.0)
    unit = aug_rows(jnp.ones((1, lanes), jnp.float32), lanes)
    for i in range(per_step):
        part = slice(i * size, (i + 1) * size)
        scores = scores_of(
            jnp.concatenate([k_ref[part, :], bias], axis=0),
            jnp.concatenate([q_ref[part, :], unit], axis=0),
        )
        top = jnp.max(scores, axis=0, keepdims=True)
        p = jnp.exp2((scores - top) * scale).astype(jnp.bfloat16)
        base = i * (size + AUG)
        out_ref[base : base + size + AUG, :] = jnp.dot(
            weighted_values(v_ref[part, :], weight), p, preferred_element_type=jnp.float32
        )
        out_ref[base + size + 1 : base + size + 2, :] = top


def rest_kernel(
    heads, scale, per_step, far_span, middle, offs, valid,
    x_ref, xp_ref, gain_ref, w_ref, q_ref, k_ref, v_ref, own_ref, ppos_ref,
    *rest,
):
    others = middle - 2
    midk, midv = rest[:others], rest[others : 2 * others]
    fark_ref, farv_ref, extra_ref, subgain_ref, wout_ref = rest[2 * others : 2 * others + 5]
    out_ref, kvp, far_t, o_scr, att = rest[2 * others + 5 :]
    rows, width = x_ref.shape
    size = width // heads
    lanes = rows // MIDDLE_DILATION
    few = rows // FAR_DILATION
    step = pl.program_id(0)

    @pl.when(step == 0)
    def _():
        project_into(kvp, xp_ref, gain_ref, w_ref, 256, width)
        for i in range(fark_ref.shape[0] // 128):
            far_t[:width, i * 128 : (i + 1) * 128] = fark_ref[i * 128 : (i + 1) * 128, :].T
            far_t[width:, i * 128 : (i + 1) * 128] = farv_ref[i * 128 : (i + 1) * 128, :].T

    me = lax.axis_index("seq")
    alive = ppos_ref[...] + (me ^ 1) * rows < valid[0]
    bias = aug_rows(jnp.where(alive, 0.0, NEGATIVE), rows)
    weight = jnp.where(alive, 1.0, 0.0)
    unit = aug_rows(jnp.ones((1, rows), jnp.float32), rows)
    is_far = extra_ref[1:2, :]
    device = extra_ref[2:3, :] ^ me
    start = extra_ref[0:1, :] + device * rows
    times = jnp.where((is_far == 1) & (device // far_span == me // far_span), 2, 1)
    lane = lax.broadcasted_iota(jnp.int32, (1, lanes), 1)
    for i in range(per_step):
        head = step * per_step + i
        part = slice(i * size, (i + 1) * size)
        base = i * (size + AUG)
        both = slice(base, base + size + AUG)
        phase = offs[head] % FAR_DILATION
        quarter = phase % MIDDLE_DILATION
        cols = pl.ds(pl.multiple_of(quarter * lanes, lanes), lanes)
        krows = pl.ds(pl.multiple_of(head * size, AUG), size)
        vrows = pl.ds(pl.multiple_of(width + head * size, AUG), size)

        scores = scores_of(
            jnp.concatenate([kvp[krows, :], bias], axis=0),
            jnp.concatenate([q_ref[part, :], unit], axis=0),
        )
        own = own_ref[both, :]
        own_top = own[size + 1 : size + 2, :]
        top = jnp.maximum(own_top, jnp.max(scores, axis=0, keepdims=True))
        p = jnp.exp2((scores - top) * scale).astype(jnp.bfloat16)
        o_scr[both, :] = own * jnp.exp2((own_top - top) * scale) + jnp.dot(
            weighted_values(kvp[vrows, :], weight), p, preferred_element_type=jnp.float32
        )
        o_scr[base + size + 1 : base + size + 2, :] = top

        keys = jnp.concatenate(
            [k_ref[part, cols], kvp[krows, cols]]
            + [midk[g][part, :] for g in range(others)]
            + [far_t[krows, :]],
            axis=1,
        )
        values = jnp.concatenate(
            [v_ref[part, cols], kvp[vrows, cols]]
            + [midv[g][part, :] for g in range(others)]
            + [far_t[vrows, :]],
            axis=1,
        )
        spot = start + jnp.where(is_far == 1, phase, quarter)
        live = spot < valid[0]
        count = jnp.where(live, times, 0).astype(jnp.float32)
        keys = jnp.concatenate(
            [
                keys,
                aug_rows(
                    jnp.where(live, 0.0, NEGATIVE), keys.shape[1], is_far.astype(jnp.float32)
                ),
            ],
            axis=0,
        )
        mine = lane // few == phase // MIDDLE_DILATION
        queries = jnp.concatenate(
            [
                q_ref[part, cols],
                aug_rows(
                    jnp.ones((1, lanes), jnp.float32), lanes, jnp.where(mine, 0.0, NEGATIVE)
                ),
            ],
            axis=0,
        )
        more = scores_of(keys, queries)
        had = o_scr[both, cols]
        had_top = had[size + 1 : size + 2, :]
        new_top = jnp.maximum(had_top, jnp.max(more, axis=0, keepdims=True))
        p = jnp.exp2((more - new_top) * scale).astype(jnp.bfloat16)
        total = had * jnp.exp2((had_top - new_top) * scale) + jnp.dot(
            weighted_values(values, count), p, preferred_element_type=jnp.float32
        )
        o_scr[both, cols] = jnp.where(new_top > 0.5 * NEGATIVE, total, 0.0)
        done = o_scr[both, :]
        result = done[:size] / jnp.maximum(done[size : size + 1], 1.0)
        att[pl.ds(pl.multiple_of(head * size, AUG), size), :] = result.astype(jnp.bfloat16)

    @pl.when(step == pl.num_programs(0) - 1)
    def _():
        attended = att[...].astype(jnp.float32)
        average = jnp.mean(attended, axis=0, keepdims=True)
        centred = attended - average
        variance = jnp.mean(centred * centred, axis=0, keepdims=True)
        normed = centred * lax.rsqrt(variance + EPSILON) * subgain_ref[...]
        projected = jnp.dot(
            normed.T.astype(jnp.bfloat16), wout_ref[...], preferred_element_type=jnp.float32
        )
        out_ref[...] = (x_ref[...].astype(jnp.float32) + projected).astype(jnp.bfloat16)


def doubled(rows, bit, devices):
    pairs = [(d, d ^ (1 << bit)) for d in range(devices)]
    return jnp.concatenate([rows, lax.ppermute(rows, "seq", pairs)], axis=0)


def gathered_body(tile_embed, valid_tiles, offsets, norm_gain, w_qkv, sub_gain, w_out):
    devices = lax.axis_size("seq")
    me = lax.axis_index("seq")
    rows, width = tile_embed.shape
    heads = offsets.shape[0]
    size = width // heads
    lanes = rows // MIDDLE_DILATION
    few = rows // FAR_DILATION
    each = rows // devices
    middle = max(4, devices // 16)
    far_span = max(8, devices // 4)
    per_step = 2
    steps = heads // per_step
    scale = float(size) ** -0.5 * LOG2E

    w_t = w_qkv.T
    pieces = tile_embed.reshape(devices, each, width)
    arrived = lax.all_to_all(pieces, "seq", split_axis=0, concat_axis=0, tiled=True)
    groups = devices // FAR_DILATION
    x = arrived.reshape(groups, 4, 4, each, width).transpose(2, 1, 0, 3, 4).reshape(rows, width)
    xp = lax.ppermute(x, "seq", [(d, d ^ 1) for d in range(devices)])

    whole = lambda *shape: pl.BlockSpec(shape, lambda *_: (0,) * len(shape))
    smem = pl.BlockSpec(memory_space=pltpu.SMEM)
    gain = norm_gain.reshape(1, width)

    proj, mid, far_key, far_value = pl.pallas_call(
        functools.partial(project_kernel, heads),
        out_shape=(
            jax.ShapeDtypeStruct((3 * width, rows), jnp.bfloat16),
            jax.ShapeDtypeStruct((2 * width, lanes), jnp.bfloat16),
            jax.ShapeDtypeStruct((few, width), jnp.bfloat16),
            jax.ShapeDtypeStruct((few, width), jnp.bfloat16),
        ),
        in_specs=[smem] + [pl.BlockSpec(memory_space=pltpu.VMEM)] * 3,
        out_specs=(pl.BlockSpec(memory_space=pltpu.VMEM),) * 4,
        scratch_shapes=[pltpu.VMEM((2 * width, lanes), jnp.float32)],
        compiler_params=pltpu.CompilerParams(vmem_limit_bytes=VMEM_LIMIT),
        cost_estimate=pl.CostEstimate(
            flops=6 * rows * width * width, bytes_accessed=12 * width * width, transcendentals=0
        ),
        name="project",
    )(offsets, x, gain, w_t)

    mids = [
        lax.ppermute(mid, "seq", [(d, d ^ g) for d in range(devices)]) for g in range(2, middle)
    ]
    bits = devices.bit_length() - 1
    for bit in range(bits):
        far_key = doubled(far_key, bit, devices)
        far_value = doubled(far_value, bits - 1 - bit, devices)
    far_value = (
        far_value.reshape((2,) * bits + (few, width))
        .transpose(tuple(reversed(range(bits))) + (bits, bits + 1))
        .reshape(devices * few, width)
    )

    local = np.arange(rows, dtype=np.int32).reshape(each, groups, 4, 4).transpose(3, 2, 1, 0)
    local = local.reshape(1, rows)
    seats = np.arange(devices, dtype=np.int32)
    mid_rows = [np.tile(local[0, :lanes], middle), np.zeros(middle * lanes, np.int32),
                np.repeat(np.arange(middle, dtype=np.int32), lanes)]
    far_rows = [np.tile(local[0, :few], devices), np.ones(devices * few, np.int32),
                np.repeat(seats, few)]
    extra = np.concatenate([np.stack(mid_rows), np.stack(far_rows)], axis=1)
    extra_count = extra.shape[1]

    strip = per_step * size
    out_strip = per_step * (size + AUG)
    block = lambda part: pl.BlockSpec((strip, rows), lambda h: (part * steps + h, 0))
    own = pl.pallas_call(
        functools.partial(own_kernel, scale, per_step, size),
        grid=(steps,),
        out_shape=jax.ShapeDtypeStruct((heads * (size + AUG), rows), jnp.float32),
        in_specs=[smem, block(0), block(1), block(2), whole(1, rows)],
        out_specs=pl.BlockSpec((out_strip, rows), lambda h: (h, 0)),
        compiler_params=pltpu.CompilerParams(vmem_limit_bytes=VMEM_LIMIT),
        cost_estimate=pl.CostEstimate(
            flops=16 * rows * rows * width, bytes_accessed=8 * rows * width,
            transcendentals=heads * rows * rows,
        ),
        name="own_keys",
    )(valid_tiles, proj, proj, proj, jnp.asarray(local))

    out = pl.pallas_call(
        functools.partial(rest_kernel, heads, scale, per_step, far_span, middle),
        grid=(steps,),
        out_shape=jax.ShapeDtypeStruct((rows, width), jnp.bfloat16),
        in_specs=[
            smem, smem,
            whole(rows, width), whole(rows, width), whole(1, width), whole(3 * width, width),
            block(0), block(1), block(2),
            pl.BlockSpec((out_strip, rows), lambda h: (h, 0)),
            whole(1, rows),
            *[pl.BlockSpec((strip, lanes), lambda h: (h, 0))] * len(mids),
            *[pl.BlockSpec((strip, lanes), lambda h: (steps + h, 0))] * len(mids),
            whole(devices * few, width), whole(devices * few, width), whole(3, extra_count),
            whole(width, 1), whole(width, width),
        ],
        out_specs=whole(rows, width),
        scratch_shapes=[
            pltpu.VMEM((2 * width, rows), jnp.bfloat16),
            pltpu.VMEM((2 * width, devices * few), jnp.bfloat16),
            pltpu.VMEM((out_strip, rows), jnp.float32),
            pltpu.VMEM((width, rows), jnp.bfloat16),
        ],
        compiler_params=pltpu.CompilerParams(vmem_limit_bytes=VMEM_LIMIT),
        cost_estimate=pl.CostEstimate(
            flops=24 * rows * rows * width, bytes_accessed=20 * rows * width,
            transcendentals=heads * rows * rows,
        ),
        name="rest",
    )(
        offsets, valid_tiles, x, xp, gain, w_t, proj, proj, proj, own, jnp.asarray(local),
        *mids, *mids, far_key, far_value, jnp.asarray(extra), sub_gain.reshape(width, 1), w_out,
    )
    return (
        out.reshape(4, 4, groups, each, width).transpose(3, 2, 1, 0, 4).reshape(rows, width)
    )


def flip(number, mask):
    for bit in range(mask.bit_length()):
        if mask >> bit & 1:
            number = number + (1 << bit) * (1 - 2 * ((number // (1 << bit)) % 2))
    return number


def to(device):
    return {"seq": device}


def remote(src, dst, send, recv, device):
    return pltpu.make_async_remote_copy(
        src_ref=src, dst_ref=dst, send_sem=send, recv_sem=recv,
        device_id=to(device), device_id_type=pl.DeviceIdType.MESH,
    )


def split_rows(total, top):
    lanes = total.shape[1]
    spot = lax.broadcasted_iota(jnp.int32, (AUG, lanes), 0)
    rounded = lambda a: a.astype(jnp.bfloat16).astype(jnp.float32)
    total_high = rounded(total)
    top_high = rounded(top)
    top_mid = rounded(top - top_high)
    parts = [total_high, total - total_high, top_high, top_mid, top - top_high - top_mid]
    rows = jnp.zeros((AUG, lanes), jnp.float32)
    for i, part in enumerate(parts):
        rows = jnp.where(spot == i, part, rows)
    return rows


def layer_kernel(
    heads, devices, scale,
    offs, valid, x_hbm, gain_ref, w_hbm, subgain_ref, wout_hbm,
    out_ref,
    xr, normed, xown, w_v, w_t, wout_v, qa, ka, va, acc, att,
    mtx, mrx, mres, mret, fmsg, frx, fres, fret,
    s1, r1, s2, r2, ms, mr, ns, nr, fs, fr, gs, gr, ws,
):
    rows, width = out_ref.shape
    size = width // heads
    half = devices // 2
    each = rows // devices
    lanes = rows // MIDDLE_DILATION
    few = rows // FAR_DILATION
    group = mrx.shape[0]
    per_group = heads // group
    pad = size + AUG
    mid_chunk = rows // 2
    me = lax.axis_index("seq")
    par = me % 2
    pair = me // 2
    partner = me + 1 - 2 * par
    seat = me % group
    base = me - seat

    load_w = pltpu.make_async_copy(w_hbm, w_v, ws.at[0])
    load_w.start()
    load_wout = pltpu.make_async_copy(wout_hbm, wout_v, ws.at[1])
    load_wout.start()
    own_block = pltpu.make_async_copy(x_hbm.at[pair], xr.at[0, pair], ws.at[2])
    own_block.start()

    barrier = pltpu.get_barrier_semaphore()
    for d in range(1, devices):
        pl.semaphore_signal(
            barrier, inc=1, device_id=to(flip(me, d)), device_id_type=pl.DeviceIdType.MESH
        )
    pl.semaphore_wait(barrier, devices - 1)

    def first(j):
        other = flip(pair, j)
        return remote(
            x_hbm.at[other], xr.at[0, pair], s1.at[j], r1.at[pair], 2 * other + par
        )

    def first_arrival(j):
        other = flip(pair, j)
        return remote(
            x_hbm.at[other], xr.at[0, other], s1.at[j], r1.at[other], 2 * other + par
        )

    def second(k):
        return remote(xr.at[0, k], xr.at[1, k], s2.at[k], r2.at[k], partner)

    for j in range(1, half):
        first(j).start()
    own_block.wait()
    second(pair).start()

    column = lax.broadcasted_iota(jnp.int32, (1, rows), 1)
    block = column // few
    side = (block // half + par) % 2
    phase = (block % 4) * 4 + ((block % half) // 4) * 2 + side
    place = (column % few) * FAR_DILATION + phase
    unit = aug_rows(jnp.ones((1, rows), jnp.float32), rows)
    alive = []
    for device in (me, partner):
        alive.append((place + device * rows < valid[0]))
    weights = [jnp.where(a, 1.0, 0.0) for a in alive]
    biases = [aug_rows(jnp.where(a, 0.0, NEGATIVE), rows) for a in alive]
    weight_rows = [aug_rows(a, rows) for a in weights]

    @pl.loop(0, heads)
    def _(h):
        qa[h, size:, :] = unit
        for m in range(2):
            ka[h, size:, m * rows : (m + 1) * rows] = biases[m]
            va[h, size:, m * rows : (m + 1) * rows] = weight_rows[m]

    load_w.wait()

    @pl.loop(0, w_v.shape[1] // 256)
    def _(i):
        cols = pl.ds(pl.multiple_of(i * 256, 256), 256)
        w_t[cols, :] = w_v[:, cols].T

    gain = gain_ref[...].reshape(1, width)

    def norm_block(side_index, k):
        spot = side_index * half + (k % 2) * (half // 2) + k // 2
        at = pl.ds(pl.multiple_of(spot * each, each), each)
        mine = xr[side_index, k, par]
        xown[at, :] = mine
        normed[0, at, :] = layer_norm_rows(mine.astype(jnp.float32), gain).astype(jnp.bfloat16)
        theirs = xr[side_index, k, 1 - par]
        normed[1, at, :] = layer_norm_rows(theirs.astype(jnp.float32), gain).astype(jnp.bfloat16)

    norm_block(0, pair)
    for j in range(1, half):
        k = flip(pair, j)
        first_arrival(j).wait_recv()
        second(k).start()
        norm_block(0, k)

    def project(c):
        at = slice(c * mid_chunk, (c + 1) * mid_chunk)
        for m in range(2):
            tokens = normed[m, at, :]
            where = slice(m * rows + c * mid_chunk, m * rows + (c + 1) * mid_chunk)
            for part in range(3):
                if m == 1 and part == 0:
                    continue
                for g in range(2):
                    count = heads // 2
                    first_row = part * width + g * count * size
                    result = lax.dot_general(
                        w_t[first_row : first_row + count * size, :], tokens,
                        (((1,), (1,)), ((), ())), preferred_element_type=jnp.float32,
                    )
                    if part == 0:
                        result = result * scale
                    if part == 2:
                        result = result * weights[m][:, at]
                    result = result.astype(jnp.bfloat16)
                    dst = (qa, ka, va)[part]
                    for i in range(count):
                        dst[g * count + i, :size, where] = result[i * size : (i + 1) * size]

    project(0)
    for j in range(half):
        k = flip(pair, j)
        second(k).wait_recv()
        norm_block(1, k)
    project(1)

    pick_row = lax.broadcasted_iota(jnp.int32, (3 * lanes, lanes), 0)
    pick_col = lax.broadcasted_iota(jnp.int32, (1, lanes), 1)
    source = jnp.where(
        pick_col < 3 * few, (pick_col // few) * lanes + pick_col % few, -devices * rows
    )

    def head_spot(h):
        turn = offs[h] % FAR_DILATION
        where = ((turn + par) % 2) * 2 + (turn // 2) % 2
        return turn, where

    all_rows = lax.broadcasted_iota(jnp.int32, (rows, lanes), 0)
    ahead = all_rows - lax.broadcasted_iota(jnp.int32, (rows, lanes), 1)

    @pl.loop(0, heads)
    def _(h):
        turn, where = head_spot(h)
        choose = jnp.where(ahead == where * lanes, 1.0, 0.0).astype(jnp.bfloat16)
        chosen = jnp.dot(
            jnp.concatenate([qa[h, :size, :], ka[h, :size, :rows], va[h, :size, :rows]], axis=0),
            choose, preferred_element_type=jnp.float32,
        ).astype(jnp.bfloat16)
        mtx[h // per_group, h % per_group] = chosen
        pick = jnp.where(pick_row == source + (turn // 4) * few, 1.0, 0.0).astype(jnp.bfloat16)
        pieces = [chosen[i * size : (i + 1) * size] for i in range(3)]
        fmsg[h] = jnp.dot(
            jnp.concatenate(pieces, axis=1), pick, preferred_element_type=jnp.float32
        ).astype(jnp.bfloat16)

    def mid_send(j):
        other = flip(seat, j)
        return remote(mtx.at[other], mrx.at[seat], ms.at[j], mr.at[seat], base + other)

    def mid_arrival(j):
        other = flip(seat, j)
        return remote(mtx.at[other], mrx.at[other], ms.at[j], mr.at[other], base + other)

    def far_send(j):
        other = flip(me, j)
        return remote(fmsg.at[other], frx.at[me], fs.at[j], fr.at[me], other)

    def far_arrival(j):
        other = flip(me, j)
        return remote(fmsg.at[other], frx.at[other], fs.at[j], fr.at[other], other)

    for j in range(1, devices):
        far_send(j).start()
    for j in range(1, group):
        mid_send(j).start()
    mrx[seat] = mtx[seat]
    frx[me] = fmsg[me]

    def attend(keys, queries, values):
        scores = scores_of(keys, queries)
        top = jnp.max(scores, axis=0, keepdims=True)
        p = jnp.exp2(scores - top).astype(jnp.bfloat16)
        return jnp.dot(values, p, preferred_element_type=jnp.float32), top

    def near(h):
        for n in range(2):
            cols = slice(n * mid_chunk, (n + 1) * mid_chunk)
            got, top = attend(ka[h], qa[h, :, cols], va[h])
            acc[h, :, cols] = got
            acc[h, size + 1 : size + 2, cols] = top

    first_heads = heads // 2

    @pl.loop(0, first_heads)
    def _(h):
        near(h)

    for j in range(1, group):
        mid_arrival(j).wait_recv()

    mid_lane = lax.broadcasted_iota(jnp.int32, (1, group * lanes), 1)
    mid_place = (
        (base + mid_lane // lanes) * rows
        + (mid_lane % few) * FAR_DILATION
        + ((mid_lane % lanes) // few) * MIDDLE_DILATION
    )

    @pl.loop(0, per_group)
    def _(i):
        quarter = offs[seat * per_group + i] % MIDDLE_DILATION
        live = mid_place + quarter < valid[0]
        joined = [
            jnp.concatenate(
                [mrx[g, i, p * size : (p + 1) * size, :] for g in range(group)], axis=1
            )
            for p in range(3)
        ]
        queries = jnp.concatenate(
            [joined[0], aug_rows(jnp.ones((1, group * lanes), jnp.float32), group * lanes)], axis=0
        )
        keys = jnp.concatenate(
            [joined[1], aug_rows(jnp.where(live, 0.0, NEGATIVE), group * lanes)], axis=0
        )
        values = jnp.concatenate(
            [joined[2], aug_rows(jnp.where(live, 1.0, 0.0), group * lanes)], axis=0
        )
        for n in range(2):
            wide = group * lanes // 2
            got, top = attend(keys, queries[:, n * wide : (n + 1) * wide], values)
            sent = jnp.concatenate(
                [got[:size], split_rows(got[size : size + 1], top)], axis=0
            ).astype(jnp.bfloat16)
            for g in range(group // 2):
                mres[n * (group // 2) + g, i] = sent[:, g * lanes : (g + 1) * lanes]

    def mid_return(j):
        other = flip(seat, j)
        return remote(mres.at[other], mret.at[seat], ns.at[j], nr.at[seat], base + other)

    def mid_returned(j):
        other = flip(seat, j)
        return remote(mres.at[other], mret.at[other], ns.at[j], nr.at[other], base + other)

    for j in range(1, group):
        mid_return(j).start()
    mret[seat] = mres[seat]

    for j in range(1, devices):
        far_arrival(j).wait_recv()

    my_turn = offs[me] % FAR_DILATION
    turned = [frx[d].T for d in range(devices)]
    far_q, far_k, far_v = (
        jnp.concatenate([t[p * few : (p + 1) * few] for t in turned], axis=0) for p in range(3)
    )
    far_row = lax.broadcasted_iota(jnp.int32, (devices * few, 1), 0)
    far_live = far_row * FAR_DILATION + my_turn < valid[0]
    far_size = devices * few // 2
    sums = lax.broadcasted_iota(jnp.int32, (devices * few, AUG), 1) == 0
    for n in range(2):
        scores = lax.dot_general(
            far_k, far_q[n * far_size : (n + 1) * far_size], (((1,), (1,)), ((), ())),
            preferred_element_type=jnp.float32,
        )
        scores = jnp.where(far_live, scores, NEGATIVE)
        top = jnp.max(scores, axis=0, keepdims=True)
        p = jnp.exp2(scores - top).astype(jnp.bfloat16)
        count = jnp.where(far_live, jnp.where(far_row // far_size == n, 2.0, 1.0), 0.0)
        numer = lax.dot_general(
            (far_v.astype(jnp.float32) * count).astype(jnp.bfloat16), p,
            (((0,), (0,)), ((), ())), preferred_element_type=jnp.float32,
        )
        total = lax.dot_general(
            jnp.where(sums, count, 0.0).astype(jnp.bfloat16), p,
            (((0,), (0,)), ((), ())), preferred_element_type=jnp.float32,
        )
        sent = jnp.concatenate(
            [numer, split_rows(total[:1], top),
             jnp.zeros((lanes - pad, far_size), jnp.float32)], axis=0,
        ).T.astype(jnp.bfloat16)
        for d in range(devices // 2):
            fres[n * (devices // 2) + d] = sent[d * few : (d + 1) * few]

    def far_return(j):
        other = flip(me, j)
        return remote(fres.at[other], fret.at[me], gs.at[j], gr.at[me], other)

    def far_returned(j):
        other = flip(me, j)
        return remote(fres.at[other], fret.at[other], gs.at[j], gr.at[other], other)

    for j in range(1, devices):
        far_return(j).start()
    fret[me] = fres[me]

    @pl.loop(first_heads, heads)
    def _(h):
        near(h)

    for j in range(1, group):
        mid_returned(j).wait_recv()
    for j in range(1, devices):
        far_returned(j).wait_recv()

    few_row = lax.broadcasted_iota(jnp.int32, (few, rows), 0)

    @pl.loop(0, heads)
    def _(h):
        turn, _ = head_spot(h)
        in_mid = phase % MIDDLE_DILATION == turn % MIDDLE_DILATION
        in_far = phase == turn
        mid = mret[h // per_group, h % per_group].astype(jnp.float32)
        mid = jnp.concatenate([mid] * (rows // lanes), axis=1)
        spread = jnp.where(in_far & (column % few == few_row), 1.0, 0.0).astype(jnp.bfloat16)
        far = lax.dot_general(
            fret[h], spread, (((0,), (0,)), ((), ())), preferred_element_type=jnp.float32
        )
        near_top = acc[h, size + 1 : size + 2, :]

        def stats(a):
            return (
                a[size : size + 1] + a[size + 1 : size + 2],
                a[size + 2 : size + 3] + a[size + 3 : size + 4] + a[size + 4 : size + 5],
            )

        mid_total, mid_top = stats(mid)
        far_total, far_top = stats(far)
        top = jnp.maximum(
            near_top,
            jnp.maximum(jnp.where(in_mid, mid_top, NEGATIVE), jnp.where(in_far, far_top, NEGATIVE)),
        )
        near_by = jnp.exp2(near_top - top)
        mid_by = jnp.where(in_mid, jnp.exp2(jnp.where(in_mid, mid_top, NEGATIVE) - top), 0.0)
        far_by = jnp.where(in_far, jnp.exp2(jnp.where(in_far, far_top, NEGATIVE) - top), 0.0)
        den = near_by * acc[h, size : size + 1, :] + mid_by * mid_total + far_by * far_total
        num = near_by * acc[h, :size, :] + mid_by * mid[:size] + far_by * far[:size]
        att[pl.ds(pl.multiple_of(h * size, AUG), size), :] = (
            num / jnp.maximum(den, 1.0)
        ).astype(jnp.bfloat16)

    load_wout.wait()
    subgain = subgain_ref[...].reshape(1, width)
    for c in range(2):
        at = slice(c * mid_chunk, (c + 1) * mid_chunk)
        target = lax.broadcasted_iota(jnp.int32, (mid_chunk, 1), 0) + c * mid_chunk
        order = jnp.where(place == target, 1.0, 0.0).astype(jnp.bfloat16)
        attended = lax.dot_general(
            order, att[...], (((1,), (1,)), ((), ())), preferred_element_type=jnp.float32
        )
        residual = jnp.dot(order, xown[...], preferred_element_type=jnp.float32)
        sub_normed = layer_norm_rows(attended, subgain).astype(jnp.bfloat16)
        out_ref[at, :] = (
            residual + jnp.dot(sub_normed, wout_v[...], preferred_element_type=jnp.float32)
        ).astype(jnp.bfloat16)

    for j in range(1, half):
        first(j).wait_send()
    for j in range(half):
        second(flip(pair, j)).wait_send()
    for j in range(1, group):
        mid_send(j).wait_send()
        mid_return(j).wait_send()
    for j in range(1, devices):
        far_send(j).wait_send()
        far_return(j).wait_send()


def exchanged_body(tile_embed, valid_tiles, offsets, norm_gain, w_qkv, sub_gain, w_out):
    devices = lax.axis_size("seq")
    rows, width = tile_embed.shape
    heads = offsets.shape[0]
    size = width // heads
    pad = size + AUG
    half = devices // 2
    each = rows // devices
    lanes = rows // MIDDLE_DILATION
    few = rows // FAR_DILATION
    group = max(4, devices // 16)
    per_group = heads // group
    scale = float(size) ** -0.5 * LOG2E
    bf16 = lambda *shape: pltpu.VMEM(shape, jnp.bfloat16)
    vmem = pl.BlockSpec(memory_space=pltpu.VMEM)
    smem = pl.BlockSpec(memory_space=pltpu.SMEM)
    anywhere = pl.BlockSpec(memory_space=pl.ANY)
    sems = lambda n: pltpu.SemaphoreType.DMA((n,))
    return pl.pallas_call(
        functools.partial(layer_kernel, heads, devices, scale),
        out_shape=jax.ShapeDtypeStruct((rows, width), jnp.bfloat16),
        in_specs=[smem, smem, anywhere, vmem, anywhere, vmem, anywhere],
        out_specs=vmem,
        scratch_shapes=[
            bf16(2, half, 2, each, width),
            bf16(2, rows, width),
            bf16(rows, width),
            bf16(*w_qkv.shape),
            bf16(*w_qkv.shape[::-1]),
            bf16(*w_out.shape),
            bf16(heads, pad, rows),
            bf16(heads, pad, 2 * rows),
            bf16(heads, pad, 2 * rows),
            pltpu.VMEM((heads, pad, rows), jnp.float32),
            bf16(width, rows),
            bf16(group, per_group, 3 * size, lanes),
            bf16(group, per_group, 3 * size, lanes),
            bf16(group, per_group, pad, lanes),
            bf16(group, per_group, pad, lanes),
            bf16(heads, size, lanes),
            bf16(devices, size, lanes),
            bf16(devices, few, lanes),
            bf16(heads, few, lanes),
            sems(half), sems(half), sems(half), sems(half),
            sems(group), sems(group), sems(group), sems(group),
            sems(devices), sems(devices), sems(devices), sems(devices),
            sems(3),
        ],
        compiler_params=pltpu.CompilerParams(
            vmem_limit_bytes=VMEM_LIMIT, collective_id=0, has_side_effects=True
        ),
        name="layer",
    )(
        offsets, valid_tiles, tile_embed.reshape(half, 2, each, width), norm_gain, w_qkv,
        sub_gain, w_out,
    )


def solution(mesh):
    devices = mesh.shape["seq"]

    def body(tile_embed, valid_tiles, offsets, *rest):
        fits = devices == offsets.shape[0] == FAR_DILATION and tile_embed.shape[0] % (16 * devices) == 0
        run = exchanged_body if fits else gathered_body
        return run(tile_embed, valid_tiles, offsets, *rest)

    return jax.shard_map(
        body,
        mesh=mesh,
        in_specs=(P(("slide", "seq"), None), P("slide"), P(), P(), P(), P(), P()),
        out_specs=P(("slide", "seq"), None),
        check_vma=False,
    )
```

```python
import functools

import jax
import jax.numpy as jnp
import numpy as np
from jax import lax
from jax.experimental import pallas as pl
from jax.experimental.pallas import tpu as pltpu
from jax.sharding import PartitionSpec as P

MIDDLE_DILATION = 4
FAR_DILATION = 16
NEGATIVE = -1e30
EPSILON = 1e-05
LOG2E = 1.4426950408889634
AUG = 16
VMEM_LIMIT = 60 * 1024 * 1024


def layer_norm_rows(x, gain):
    average = jnp.mean(x, axis=-1, keepdims=True)
    centred = x - average
    variance = jnp.mean(centred * centred, axis=-1, keepdims=True)
    return centred * lax.rsqrt(variance + EPSILON) * gain


def project_into(dst, x_ref, gain_ref, w_ref, chunk, skip=0):
    normed = layer_norm_rows(x_ref[...].astype(jnp.float32), gain_ref[...]).astype(jnp.bfloat16)

    @pl.loop(0, (w_ref.shape[0] - skip) // chunk)
    def _(i):
        rows = pl.ds(pl.multiple_of(i * chunk, chunk), chunk)
        dst[rows, :] = lax.dot_general(
            w_ref[pl.ds(pl.multiple_of(i * chunk + skip, chunk), chunk), :], normed, (((1,), (1,)), ((), ())), preferred_element_type=jnp.float32
        ).astype(jnp.bfloat16)


def project_kernel(heads, offs, x_ref, gain_ref, w_ref, proj_ref, mid_ref, fark_ref, farv_ref, far_scr):
    rows, width = x_ref.shape
    size = width // heads
    lanes = rows // MIDDLE_DILATION
    few = rows // FAR_DILATION
    project_into(proj_ref, x_ref, gain_ref, w_ref, 256)
    src = lax.broadcasted_iota(jnp.int32, (lanes, lanes), 0)
    dst = lax.broadcasted_iota(jnp.int32, (lanes, lanes), 1)
    for head in range(heads):
        phase = offs[head] % FAR_DILATION
        quarter = phase % MIDDLE_DILATION
        shift = (phase // MIDDLE_DILATION) * few
        pick = ((src == dst + shift) & (dst < few)).astype(jnp.bfloat16)
        for part in range(2):
            base = part * width + head * size
            block = proj_ref[
                width + base : width + base + size,
                pl.ds(pl.multiple_of(quarter * lanes, lanes), lanes),
            ]
            mid_ref[base : base + size, :] = block
            far_scr[base : base + size, :] = jnp.dot(
                block, pick, preferred_element_type=jnp.float32
            )
    fark_ref[...] = far_scr[:width, :].T[:few].astype(jnp.bfloat16)
    farv_ref[...] = far_scr[width:, :].T[:few].astype(jnp.bfloat16)


def aug_rows(first, lanes, second=None):
    spot = lax.broadcasted_iota(jnp.int32, (AUG, lanes), 0)
    rows = jnp.where(spot == 0, first, 0.0)
    if second is not None:
        rows = jnp.where(spot == 1, second, rows)
    return rows.astype(jnp.bfloat16)


def weighted_values(value, weight):
    scaled = (value.astype(jnp.float32) * weight).astype(jnp.bfloat16)
    return jnp.concatenate([scaled, aug_rows(weight, value.shape[1])], axis=0)


def scores_of(keys, queries):
    return lax.dot_general(
        keys, queries, (((0,), (0,)), ((), ())), preferred_element_type=jnp.float32
    )


def own_kernel(scale, per_step, size, valid, q_ref, k_ref, v_ref, pos_ref, out_ref):
    lanes = q_ref.shape[1]
    alive = pos_ref[...] + lax.axis_index("seq") * lanes < valid[0]
    bias = aug_rows(jnp.where(alive, 0.0, NEGATIVE), lanes)
    weight = jnp.where(alive, 1.0, 0.0)
    unit = aug_rows(jnp.ones((1, lanes), jnp.float32), lanes)
    for i in range(per_step):
        part = slice(i * size, (i + 1) * size)
        scores = scores_of(
            jnp.concatenate([k_ref[part, :], bias], axis=0),
            jnp.concatenate([q_ref[part, :], unit], axis=0),
        )
        top = jnp.max(scores, axis=0, keepdims=True)
        p = jnp.exp2((scores - top) * scale).astype(jnp.bfloat16)
        base = i * (size + AUG)
        out_ref[base : base + size + AUG, :] = jnp.dot(
            weighted_values(v_ref[part, :], weight), p, preferred_element_type=jnp.float32
        )
        out_ref[base + size + 1 : base + size + 2, :] = top


def rest_kernel(
    heads, scale, per_step, far_span, middle, offs, valid,
    x_ref, xp_ref, gain_ref, w_ref, q_ref, k_ref, v_ref, own_ref, ppos_ref,
    *rest,
):
    others = middle - 2
    midk, midv = rest[:others], rest[others : 2 * others]
    fark_ref, farv_ref, extra_ref, subgain_ref, wout_ref = rest[2 * others : 2 * others + 5]
    out_ref, kvp, far_t, o_scr, att = rest[2 * others + 5 :]
    rows, width = x_ref.shape
    size = width // heads
    lanes = rows // MIDDLE_DILATION
    few = rows // FAR_DILATION
    step = pl.program_id(0)

    @pl.when(step == 0)
    def _():
        project_into(kvp, xp_ref, gain_ref, w_ref, 256, width)
        for i in range(fark_ref.shape[0] // 128):
            far_t[:width, i * 128 : (i + 1) * 128] = fark_ref[i * 128 : (i + 1) * 128, :].T
            far_t[width:, i * 128 : (i + 1) * 128] = farv_ref[i * 128 : (i + 1) * 128, :].T

    me = lax.axis_index("seq")
    alive = ppos_ref[...] + (me ^ 1) * rows < valid[0]
    bias = aug_rows(jnp.where(alive, 0.0, NEGATIVE), rows)
    weight = jnp.where(alive, 1.0, 0.0)
    unit = aug_rows(jnp.ones((1, rows), jnp.float32), rows)
    is_far = extra_ref[1:2, :]
    device = extra_ref[2:3, :] ^ me
    start = extra_ref[0:1, :] + device * rows
    times = jnp.where((is_far == 1) & (device // far_span == me // far_span), 2, 1)
    lane = lax.broadcasted_iota(jnp.int32, (1, lanes), 1)
    for i in range(per_step):
        head = step * per_step + i
        part = slice(i * size, (i + 1) * size)
        base = i * (size + AUG)
        both = slice(base, base + size + AUG)
        phase = offs[head] % FAR_DILATION
        quarter = phase % MIDDLE_DILATION
        cols = pl.ds(pl.multiple_of(quarter * lanes, lanes), lanes)
        krows = pl.ds(pl.multiple_of(head * size, AUG), size)
        vrows = pl.ds(pl.multiple_of(width + head * size, AUG), size)

        scores = scores_of(
            jnp.concatenate([kvp[krows, :], bias], axis=0),
            jnp.concatenate([q_ref[part, :], unit], axis=0),
        )
        own = own_ref[both, :]
        own_top = own[size + 1 : size + 2, :]
        top = jnp.maximum(own_top, jnp.max(scores, axis=0, keepdims=True))
        p = jnp.exp2((scores - top) * scale).astype(jnp.bfloat16)
        o_scr[both, :] = own * jnp.exp2((own_top - top) * scale) + jnp.dot(
            weighted_values(kvp[vrows, :], weight), p, preferred_element_type=jnp.float32
        )
        o_scr[base + size + 1 : base + size + 2, :] = top

        keys = jnp.concatenate(
            [k_ref[part, cols], kvp[krows, cols]]
            + [midk[g][part, :] for g in range(others)]
            + [far_t[krows, :]],
            axis=1,
        )
        values = jnp.concatenate(
            [v_ref[part, cols], kvp[vrows, cols]]
            + [midv[g][part, :] for g in range(others)]
            + [far_t[vrows, :]],
            axis=1,
        )
        spot = start + jnp.where(is_far == 1, phase, quarter)
        live = spot < valid[0]
        count = jnp.where(live, times, 0).astype(jnp.float32)
        keys = jnp.concatenate(
            [
                keys,
                aug_rows(
                    jnp.where(live, 0.0, NEGATIVE), keys.shape[1], is_far.astype(jnp.float32)
                ),
            ],
            axis=0,
        )
        mine = lane // few == phase // MIDDLE_DILATION
        queries = jnp.concatenate(
            [
                q_ref[part, cols],
                aug_rows(
                    jnp.ones((1, lanes), jnp.float32), lanes, jnp.where(mine, 0.0, NEGATIVE)
                ),
            ],
            axis=0,
        )
        more = scores_of(keys, queries)
        had = o_scr[both, cols]
        had_top = had[size + 1 : size + 2, :]
        new_top = jnp.maximum(had_top, jnp.max(more, axis=0, keepdims=True))
        p = jnp.exp2((more - new_top) * scale).astype(jnp.bfloat16)
        total = had * jnp.exp2((had_top - new_top) * scale) + jnp.dot(
            weighted_values(values, count), p, preferred_element_type=jnp.float32
        )
        o_scr[both, cols] = jnp.where(new_top > 0.5 * NEGATIVE, total, 0.0)
        done = o_scr[both, :]
        result = done[:size] / jnp.maximum(done[size : size + 1], 1.0)
        att[pl.ds(pl.multiple_of(head * size, AUG), size), :] = result.astype(jnp.bfloat16)

    @pl.when(step == pl.num_programs(0) - 1)
    def _():
        attended = att[...].astype(jnp.float32)
        average = jnp.mean(attended, axis=0, keepdims=True)
        centred = attended - average
        variance = jnp.mean(centred * centred, axis=0, keepdims=True)
        normed = centred * lax.rsqrt(variance + EPSILON) * subgain_ref[...]
        projected = jnp.dot(
            normed.T.astype(jnp.bfloat16), wout_ref[...], preferred_element_type=jnp.float32
        )
        out_ref[...] = (x_ref[...].astype(jnp.float32) + projected).astype(jnp.bfloat16)


def doubled(rows, bit, devices):
    pairs = [(d, d ^ (1 << bit)) for d in range(devices)]
    return jnp.concatenate([rows, lax.ppermute(rows, "seq", pairs)], axis=0)


def gathered_body(tile_embed, valid_tiles, offsets, norm_gain, w_qkv, sub_gain, w_out):
    devices = lax.axis_size("seq")
    me = lax.axis_index("seq")
    rows, width = tile_embed.shape
    heads = offsets.shape[0]
    size = width // heads
    lanes = rows // MIDDLE_DILATION
    few = rows // FAR_DILATION
    each = rows // devices
    middle = max(4, devices // 16)
    far_span = max(8, devices // 4)
    per_step = 2
    steps = heads // per_step
    scale = float(size) ** -0.5 * LOG2E

    w_t = w_qkv.T
    pieces = tile_embed.reshape(devices, each, width)
    arrived = lax.all_to_all(pieces, "seq", split_axis=0, concat_axis=0, tiled=True)
    groups = devices // FAR_DILATION
    x = arrived.reshape(groups, 4, 4, each, width).transpose(2, 1, 0, 3, 4).reshape(rows, width)
    xp = lax.ppermute(x, "seq", [(d, d ^ 1) for d in range(devices)])

    whole = lambda *shape: pl.BlockSpec(shape, lambda *_: (0,) * len(shape))
    smem = pl.BlockSpec(memory_space=pltpu.SMEM)
    gain = norm_gain.reshape(1, width)

    proj, mid, far_key, far_value = pl.pallas_call(
        functools.partial(project_kernel, heads),
        out_shape=(
            jax.ShapeDtypeStruct((3 * width, rows), jnp.bfloat16),
            jax.ShapeDtypeStruct((2 * width, lanes), jnp.bfloat16),
            jax.ShapeDtypeStruct((few, width), jnp.bfloat16),
            jax.ShapeDtypeStruct((few, width), jnp.bfloat16),
        ),
        in_specs=[smem] + [pl.BlockSpec(memory_space=pltpu.VMEM)] * 3,
        out_specs=(pl.BlockSpec(memory_space=pltpu.VMEM),) * 4,
        scratch_shapes=[pltpu.VMEM((2 * width, lanes), jnp.float32)],
        compiler_params=pltpu.CompilerParams(vmem_limit_bytes=VMEM_LIMIT),
        cost_estimate=pl.CostEstimate(
            flops=6 * rows * width * width, bytes_accessed=12 * width * width, transcendentals=0
        ),
        name="project",
    )(offsets, x, gain, w_t)

    mids = [
        lax.ppermute(mid, "seq", [(d, d ^ g) for d in range(devices)]) for g in range(2, middle)
    ]
    bits = devices.bit_length() - 1
    for bit in range(bits):
        far_key = doubled(far_key, bit, devices)
        far_value = doubled(far_value, bits - 1 - bit, devices)
    far_value = (
        far_value.reshape((2,) * bits + (few, width))
        .transpose(tuple(reversed(range(bits))) + (bits, bits + 1))
        .reshape(devices * few, width)
    )

    local = np.arange(rows, dtype=np.int32).reshape(each, groups, 4, 4).transpose(3, 2, 1, 0)
    local = local.reshape(1, rows)
    seats = np.arange(devices, dtype=np.int32)
    mid_rows = [np.tile(local[0, :lanes], middle), np.zeros(middle * lanes, np.int32),
                np.repeat(np.arange(middle, dtype=np.int32), lanes)]
    far_rows = [np.tile(local[0, :few], devices), np.ones(devices * few, np.int32),
                np.repeat(seats, few)]
    extra = np.concatenate([np.stack(mid_rows), np.stack(far_rows)], axis=1)
    extra_count = extra.shape[1]

    strip = per_step * size
    out_strip = per_step * (size + AUG)
    block = lambda part: pl.BlockSpec((strip, rows), lambda h: (part * steps + h, 0))
    own = pl.pallas_call(
        functools.partial(own_kernel, scale, per_step, size),
        grid=(steps,),
        out_shape=jax.ShapeDtypeStruct((heads * (size + AUG), rows), jnp.float32),
        in_specs=[smem, block(0), block(1), block(2), whole(1, rows)],
        out_specs=pl.BlockSpec((out_strip, rows), lambda h: (h, 0)),
        compiler_params=pltpu.CompilerParams(vmem_limit_bytes=VMEM_LIMIT),
        cost_estimate=pl.CostEstimate(
            flops=16 * rows * rows * width, bytes_accessed=8 * rows * width,
            transcendentals=heads * rows * rows,
        ),
        name="own_keys",
    )(valid_tiles, proj, proj, proj, jnp.asarray(local))

    out = pl.pallas_call(
        functools.partial(rest_kernel, heads, scale, per_step, far_span, middle),
        grid=(steps,),
        out_shape=jax.ShapeDtypeStruct((rows, width), jnp.bfloat16),
        in_specs=[
            smem, smem,
            whole(rows, width), whole(rows, width), whole(1, width), whole(3 * width, width),
            block(0), block(1), block(2),
            pl.BlockSpec((out_strip, rows), lambda h: (h, 0)),
            whole(1, rows),
            *[pl.BlockSpec((strip, lanes), lambda h: (h, 0))] * len(mids),
            *[pl.BlockSpec((strip, lanes), lambda h: (steps + h, 0))] * len(mids),
            whole(devices * few, width), whole(devices * few, width), whole(3, extra_count),
            whole(width, 1), whole(width, width),
        ],
        out_specs=whole(rows, width),
        scratch_shapes=[
            pltpu.VMEM((2 * width, rows), jnp.bfloat16),
            pltpu.VMEM((2 * width, devices * few), jnp.bfloat16),
            pltpu.VMEM((out_strip, rows), jnp.float32),
            pltpu.VMEM((width, rows), jnp.bfloat16),
        ],
        compiler_params=pltpu.CompilerParams(vmem_limit_bytes=VMEM_LIMIT),
        cost_estimate=pl.CostEstimate(
            flops=24 * rows * rows * width, bytes_accessed=20 * rows * width,
            transcendentals=heads * rows * rows,
        ),
        name="rest",
    )(
        offsets, valid_tiles, x, xp, gain, w_t, proj, proj, proj, own, jnp.asarray(local),
        *mids, *mids, far_key, far_value, jnp.asarray(extra), sub_gain.reshape(width, 1), w_out,
    )
    return (
        out.reshape(4, 4, groups, each, width).transpose(3, 2, 1, 0, 4).reshape(rows, width)
    )


def flip(number, mask):
    for bit in range(mask.bit_length()):
        if mask >> bit & 1:
            number = number + (1 << bit) * (1 - 2 * ((number // (1 << bit)) % 2))
    return number


def to(device):
    return {"seq": device}


def remote(src, dst, send, recv, device):
    return pltpu.make_async_remote_copy(
        src_ref=src, dst_ref=dst, send_sem=send, recv_sem=recv,
        device_id=to(device), device_id_type=pl.DeviceIdType.MESH,
    )


def split_rows(total, top):
    lanes = total.shape[1]
    spot = lax.broadcasted_iota(jnp.int32, (AUG, lanes), 0)
    rounded = lambda a: a.astype(jnp.bfloat16).astype(jnp.float32)
    total_high = rounded(total)
    top_high = rounded(top)
    top_mid = rounded(top - top_high)
    parts = [total_high, total - total_high, top_high, top_mid, top - top_high - top_mid]
    rows = jnp.zeros((AUG, lanes), jnp.float32)
    for i, part in enumerate(parts):
        rows = jnp.where(spot == i, part, rows)
    return rows


def layer_kernel(
    heads, devices, scale,
    offs, valid, x_hbm, gain_ref, w_hbm, subgain_ref, wout_hbm,
    out_ref,
    xr, normed, w_v, w_t, wout_v, qkv, acc, att, bank, s_even, s_odd, t_even, t_odd,
    mq, mqrx, mk, mv, mloc, mres, mret, fmsg, frx, fq, fk, fv, fres, fret,
    s1, r1, s2, r2, s3, r3, ms, mr, ns, nr, fs, fr, gs, gr, ws,
):
    rows, width = out_ref.shape
    size = width // heads
    half = devices // 2
    each = rows // devices
    lanes = rows // MIDDLE_DILATION
    few = rows // FAR_DILATION
    pad = size + AUG
    wide = rows // 2
    batch = 4
    handle_at = heads // 4 - 1
    batches = heads // batch
    me = lax.axis_index("seq")
    par = me % 2
    pair = me // 2
    partner = flip(me, 1)
    across = flip(me, 2)

    seat_of = lambda k: (k % 2) * (half // 2) + k // 2
    load_w = pltpu.make_async_copy(w_hbm, w_v, ws.at[0])
    load_w.start()
    load_wout = pltpu.make_async_copy(wout_hbm, wout_v, ws.at[1])
    load_wout.start()
    own_block = pltpu.make_async_copy(x_hbm.at[pair], xr.at[0, :, seat_of(pair)], ws.at[2])
    own_block.start()

    barrier = pltpu.get_barrier_semaphore()
    for d in range(1, devices):
        pl.semaphore_signal(
            barrier, inc=1, device_id=to(flip(me, d)), device_id_type=pl.DeviceIdType.MESH
        )
    pl.semaphore_wait(barrier, devices - 1)

    def first(j):
        other = flip(pair, j)
        return remote(
            x_hbm.at[other], xr.at[0, :, seat_of(pair)], s1.at[j], r1.at[pair], 2 * other + par
        )

    def first_arrival(j):
        other = flip(pair, j)
        return remote(
            x_hbm.at[other], xr.at[0, :, seat_of(other)], s1.at[j], r1.at[other], 2 * other + par
        )

    def forward(j, member, arrives, send, recv):
        k = flip(pair, j)
        return remote(
            xr.at[0, member, seat_of(k)], xr.at[1, arrives, seat_of(k)],
            send.at[j], recv.at[k], partner,
        )

    def urgent(j):
        return forward(j, 1 - par, 1 - par, s2, r2)

    def urgent_arrival(j):
        return forward(j, 1 - par, par, s2, r2)

    def later(j):
        return forward(j, par, par, s3, r3)

    def later_arrival(j):
        return forward(j, par, 1 - par, s3, r3)

    for j in range(1, half):
        first(j).start()
    own_block.wait()
    urgent(0).start()
    later(0).start()

    column = lax.broadcasted_iota(jnp.int32, (1, rows), 1)
    block = column // few
    side = (block // half + par) % 2
    phase = (block % 4) * 4 + ((block % half) // 4) * 2 + side
    place = (column % few) * FAR_DILATION + phase
    unit = aug_rows(jnp.ones((1, rows), jnp.float32), rows)
    alive = [place + device * rows < valid[0] for device in (me, partner)]
    biases = [aug_rows(jnp.where(a, 0.0, NEGATIVE), rows) for a in alive]
    weight_rows = [aug_rows(jnp.where(a, 1.0, 0.0), rows) for a in alive]

    @pl.loop(0, heads)
    def _(h):
        qkv[h, size:, :rows] = unit
        for m in range(2):
            qkv[heads + h, size:, m * rows : (m + 1) * rows] = biases[m]
            qkv[2 * heads + h, size:, m * rows : (m + 1) * rows] = weight_rows[m]

    bank_row = lax.broadcasted_iota(jnp.int32, (3 * lanes, 1), 0)
    bank_col = lax.broadcasted_iota(jnp.int32, (1, batch * lanes), 1)
    spot = bank_col % lanes
    source = jnp.where(
        spot < 3 * few, (spot // few) * lanes + (bank_col // lanes) * few + spot % few, -1
    )
    bank[...] = jnp.where(bank_row == source, 1.0, 0.0).astype(jnp.bfloat16)

    load_w.wait()

    @pl.loop(0, w_v.shape[1] // 256)
    def _(i):
        cols = pl.ds(pl.multiple_of(i * 256, 256), 256)
        w_t[cols, :] = w_v[:, cols].T

    gain = gain_ref[...].reshape(1, width)

    def norm(m, c, first_seat, seats):
        count = seats * each
        piece = xr[c, par + m - 2 * par * m, pl.ds(first_seat, seats)]
        piece = piece.reshape(count, width).astype(jnp.float32)
        at = pl.ds(pl.multiple_of(c * wide + first_seat * each, count), count)
        normed[m, at, :] = layer_norm_rows(piece, gain).astype(jnp.bfloat16)

    quarter_seats = half // 4
    zone = (pair // 2) // quarter_seats
    for g in range(2):
        for j in range(max(1, g * half // 2), (g + 1) * half // 2):
            first_arrival(j).wait_recv()
            urgent(j).start()
            if g == 0:
                later(j).start()
        z = zone if g == 0 else 1 - zone

        @pl.loop(0, 4)
        def _(t):
            norm(t // 2, 0, (t % 2) * (half // 2) + z * quarter_seats, quarter_seats)

    for j in range(half // 2, half):
        later(j).start()

    def project(c, start, stop):
        @pl.loop(start, stop)
        def _(t):
            m = t // 3
            part = t - 2 * m
            at = slice(c * wide, (c + 1) * wide)
            device = me + m * (partner - me)
            weight = jnp.where(place[:, at] + device * rows < valid[0], 1.0, 0.0)
            part_row = jnp.zeros((1, wide), jnp.int32) + part
            factor = jnp.where(part_row == 0, scale, jnp.where(part_row == 2, weight, 1.0))
            result = lax.dot_general(
                w_t[pl.ds(pl.multiple_of(part * width, width), width), :], normed[m, at, :],
                (((1,), (1,)), ((), ())), preferred_element_type=jnp.float32,
            )
            result = (result * factor).astype(jnp.bfloat16)
            where = pl.ds(pl.multiple_of(m * rows + c * wide, wide), wide)
            for i in range(heads):
                qkv[part * heads + i, :size, where] = result[i * size : (i + 1) * size]

    project(0, 0, 5)
    for j in range(half):
        urgent_arrival(j).wait_recv()

    @pl.loop(0, 4)
    def _(t):
        norm(0, 1, t * quarter_seats, quarter_seats)

    project(1, 0, 3)

    def head_turn(h):
        turn = offs[h] % FAR_DILATION
        return turn, ((turn + par) % 2) * 2 + (turn // 2) % 2

    ones = jnp.zeros((1, lanes), jnp.int32)

    def chosen(row, shift, where):
        total = None
        for b in range(MIDDLE_DILATION):
            by = jnp.where(ones + where == b, 1.0, 0.0).astype(jnp.bfloat16)
            piece = qkv[row, :size, shift + b * lanes : shift + (b + 1) * lanes] * by
            total = piece if total is None else total + piece
        return total

    @pl.loop(0, batches)
    def _(c):
        turns = [head_turn(c * batch + i) for i in range(batch)]
        stacked = []
        for i in range(batch):
            h = c * batch + i
            pieces = [chosen(p * heads + h, 0, turns[i][1]) for p in range(3)]
            mq[c, i, :size] = pieces[0]
            mk[h, :size, :lanes] = pieces[1]
            mv[h, :size, :lanes] = pieces[2]
            stacked.append(jnp.concatenate(pieces, axis=1))
        spread = jnp.dot(
            jnp.concatenate(stacked, axis=0), bank[...], preferred_element_type=jnp.float32
        )
        for i in range(batch):
            total = None
            for b in range(4):
                by = jnp.where(ones + turns[i][0] // 4 == b, 1.0, 0.0)
                piece = spread[i * size : (i + 1) * size, b * lanes : (b + 1) * lanes] * by
                total = piece if total is None else total + piece
            fmsg[c * batch + i] = total.astype(jnp.bfloat16)

    def far_send(j):
        other = flip(me, j)
        return remote(fmsg.at[other], frx.at[me], fs.at[j], fr.at[me], other)

    def far_arrival(j):
        other = flip(me, j)
        return remote(fmsg.at[other], frx.at[other], fs.at[j], fr.at[other], other)

    def mid_send(c):
        return remote(mq.at[c], mqrx.at[c], ms.at[c], mr.at[c], across)

    def mid_return(c):
        return remote(mres.at[c], mret.at[c], ns.at[c], nr.at[c], across)

    for j in range(devices - 1, 0, -1):
        far_send(j).start()
    for c in range(batches):
        mid_send(c).start()
    frx[me] = fmsg[me]

    def attend(keys, queries, values):
        scores = scores_of(keys, queries)
        top = jnp.max(scores, axis=0, keepdims=True)
        p = jnp.exp2(scores - top).astype(jnp.bfloat16)
        return jnp.dot(values, p, preferred_element_type=jnp.float32), top

    for j in range(half):
        later_arrival(j).wait_recv()

    @pl.loop(0, 4)
    def _(t):
        norm(1, 1, t * quarter_seats, quarter_seats)

    project(1, 3, 5)

    mid_lane = lax.broadcasted_iota(jnp.int32, (1, 2 * lanes), 1)
    mid_place = (
        jnp.where(mid_lane < lanes, me, partner) * rows
        + (mid_lane % few) * FAR_DILATION
        + ((mid_lane % lanes) // few) * MIDDLE_DILATION
    )
    mid_unit = aug_rows(jnp.ones((1, 2 * lanes), jnp.float32), 2 * lanes)

    @pl.loop(0, batches)
    def _(c):
        for i in range(batch):
            h = c * batch + i
            turn, where = head_turn(h)
            mk[h, :size, lanes:] = chosen(heads + h, rows, where)
            mv[h, :size, lanes:] = chosen(2 * heads + h, rows, where)
            live = mid_place + turn % MIDDLE_DILATION < valid[0]
            mk[h, size:, :] = aug_rows(jnp.where(live, 0.0, NEGATIVE), 2 * lanes)
            mv[h, size:, :] = aug_rows(jnp.where(live, 1.0, 0.0), 2 * lanes)

    def far_return(j):
        other = flip(me, j)
        return remote(fres.at[other], fret.at[me], gs.at[j], gr.at[me], other)

    def far_returned(j):
        other = flip(me, j)
        return remote(fres.at[other], fret.at[other], gs.at[j], gr.at[other], other)

    def far_and_middle():
        for j in range(1, devices):
            far_arrival(j).wait_recv()

        @pl.loop(0, devices // 4)
        def _(g):
            for i in range(4):
                turned = frx[4 * g + i].T
                at = pl.ds(pl.multiple_of((4 * g + i) * few, few), few)
                for p, ref in enumerate((fq, fk, fv)):
                    ref[at, :] = turned[p * few : (p + 1) * few]

        my_turn = offs[me] % FAR_DILATION
        far_size = devices * few // 2
        far_row = lax.broadcasted_iota(jnp.int32, (devices * few, 1), 0)
        far_live = far_row * FAR_DILATION + my_turn < valid[0]
        sums = lax.broadcasted_iota(jnp.int32, (devices * few, AUG), 1) == 0

        @pl.loop(0, 2)
        def _(n):
            scores = lax.dot_general(
                fk[...], fq[pl.ds(pl.multiple_of(n * far_size, far_size), far_size), :],
                (((1,), (1,)), ((), ())), preferred_element_type=jnp.float32,
            )
            scores = jnp.where(far_live, scores, NEGATIVE)
            top = jnp.max(scores, axis=0, keepdims=True)
            p = jnp.exp2(scores - top).astype(jnp.bfloat16)
            count = jnp.where(far_live, jnp.where(far_row // far_size == n, 2.0, 1.0), 0.0)
            numer = lax.dot_general(
                (fv[...].astype(jnp.float32) * count).astype(jnp.bfloat16), p,
                (((0,), (0,)), ((), ())), preferred_element_type=jnp.float32,
            )
            total = lax.dot_general(
                jnp.where(sums, count, 0.0).astype(jnp.bfloat16), p,
                (((0,), (0,)), ((), ())), preferred_element_type=jnp.float32,
            )
            sent = jnp.concatenate(
                [numer, split_rows(total[:1], top),
                 jnp.zeros((lanes - pad, far_size), jnp.float32)], axis=0,
            ).T.astype(jnp.bfloat16)
            for d in range(devices // 2):
                fres[n * (devices // 2) + d] = sent[d * few : (d + 1) * few]

        for j in range(devices - 1, 0, -1):
            far_return(j).start()
        fret[me] = fres[me]

        @pl.loop(0, batches)
        def _(c):
            mid_send(c).wait_recv()
            for i in range(batch):
                h = c * batch + i
                queries = jnp.concatenate(
                    [jnp.concatenate([mq[c, i], mqrx[c, i]], axis=1), mid_unit], axis=0
                )
                got, top = attend(mk[h], queries, mv[h])
                mloc[h] = got[:, :lanes]
                mloc[h, size + 1 : size + 2, :] = top[:, :lanes]
                mres[c, i] = jnp.concatenate(
                    [got[:size, lanes:], split_rows(got[size : size + 1, lanes:], top[:, lanes:])],
                    axis=0,
                ).astype(jnp.bfloat16)
            mid_return(c).start()

    key_chunk = rows
    key_chunks = 2 * rows // key_chunk

    def scores_chunk(h, c, dst, best):
        at = slice(c * key_chunk, (c + 1) * key_chunk)
        scores = scores_of(qkv[heads + h, :, at], qkv[h, :, :rows])
        dst[at, :] = scores
        found = jnp.max(scores.reshape(key_chunk // 8, 8, rows), axis=0)
        return found if best is None else jnp.maximum(best, found)

    best = None
    for c in range(key_chunks):
        best = scores_chunk(0, c, s_even, best)
    t_even[...] = jnp.max(best, axis=0, keepdims=True)

    @pl.loop(0, heads // 2)
    def _(i):
        for u, (now, later_s, top_ref, next_top) in enumerate(
            ((s_even, s_odd, t_even, t_odd), (s_odd, s_even, t_odd, t_even))
        ):
            h = 2 * i + u
            following = 2 * i + 1 if u == 0 else (2 * i + 2) % heads
            top = top_ref[...]
            best = None
            total = None
            for c in range(key_chunks):
                at = slice(c * key_chunk, (c + 1) * key_chunk)
                best = scores_chunk(following, c, later_s, best)
                p = jnp.exp2(now[at, :] - top).astype(jnp.bfloat16)
                part = jnp.dot(qkv[2 * heads + h, :, at], p, preferred_element_type=jnp.float32)
                total = part if total is None else total + part
            acc[h] = total
            acc[h, size + 1 : size + 2, :] = top
            next_top[...] = jnp.max(best, axis=0, keepdims=True)

        @pl.when(i == handle_at)
        def _():
            far_and_middle()

    for c in range(batches):
        mid_return(c).wait_recv()
    for j in range(1, devices):
        far_returned(j).wait_recv()

    few_row = lax.broadcasted_iota(jnp.int32, (few, rows), 0)
    even = column % few == few_row

    def stats(a):
        return (
            a[size : size + 1] + a[size + 1 : size + 2],
            a[size + 2 : size + 3] + a[size + 3 : size + 4] + a[size + 4 : size + 5],
        )

    def merge(c, i):
        h = c * batch + i
        turn, _ = head_turn(h)
        in_mid = phase % MIDDLE_DILATION == turn % MIDDLE_DILATION
        in_far = phase == turn
        back = mret[c, i].astype(jnp.float32)
        back_total, back_top = stats(back)
        local_top = mloc[h, size + 1 : size + 2, :]
        mid_top = jnp.maximum(local_top, back_top)
        local_by = jnp.exp2(local_top - mid_top)
        back_by = jnp.exp2(back_top - mid_top)
        mid_total = local_by * mloc[h, size : size + 1, :] + back_by * back_total
        mid_numer = local_by * mloc[h, :size, :] + back_by * back[:size]
        over = lambda a: jnp.concatenate([a] * (rows // lanes), axis=1)
        mid_top = jnp.where(in_mid, over(mid_top), NEGATIVE)
        spread = jnp.where(in_far & even, 1.0, 0.0).astype(jnp.bfloat16)
        far = lax.dot_general(
            fret[h], spread, (((0,), (0,)), ((), ())), preferred_element_type=jnp.float32
        )
        far_total, far_top = stats(far)
        far_top = jnp.where(in_far, far_top, NEGATIVE)
        near_top = acc[h, size + 1 : size + 2, :]
        top = jnp.maximum(near_top, jnp.maximum(mid_top, far_top))
        near_by = jnp.exp2(near_top - top)
        mid_by = jnp.where(in_mid, jnp.exp2(mid_top - top), 0.0)
        far_by = jnp.where(in_far, jnp.exp2(far_top - top), 0.0)
        den = near_by * acc[h, size : size + 1, :] + mid_by * over(mid_total) + far_by * far_total
        inverse = 1.0 / jnp.maximum(den, 1.0)
        numer = (
            (near_by * inverse) * acc[h, :size, :]
            + (mid_by * inverse) * over(mid_numer)
            + (far_by * inverse) * far[:size]
        )
        att[pl.ds(pl.multiple_of(h * size, AUG), size), :] = numer.astype(jnp.bfloat16)

    @pl.loop(0, batches)
    def _(c):
        for i in range(batch):
            merge(c, i)

    load_wout.wait()
    subgain = subgain_ref[...].reshape(1, width)
    @pl.loop(0, 2)
    def _(c):
        target = lax.broadcasted_iota(jnp.int32, (wide, 1), 0) + c * wide
        order = jnp.where(place == target, 1.0, 0.0).astype(jnp.bfloat16)
        attended = lax.dot_general(
            order, att[...], (((1,), (1,)), ((), ())), preferred_element_type=jnp.float32
        )
        residual = jnp.dot(order[:, :wide], xr[0, par].reshape(wide, width), preferred_element_type=jnp.float32)
        residual += jnp.dot(order[:, wide:], xr[1, par].reshape(wide, width), preferred_element_type=jnp.float32)
        sub_normed = layer_norm_rows(attended, subgain).astype(jnp.bfloat16)
        out_ref[pl.ds(pl.multiple_of(c * wide, wide), wide), :] = (
            residual + jnp.dot(sub_normed, wout_v[...], preferred_element_type=jnp.float32)
        ).astype(jnp.bfloat16)

    for j in range(1, half):
        first(j).wait_send()
    for j in range(half):
        urgent(j).wait_send()
        later(j).wait_send()
    for c in range(batches):
        mid_send(c).wait_send()
        mid_return(c).wait_send()
    for j in range(1, devices):
        far_send(j).wait_send()
        far_return(j).wait_send()


def exchanged_body(tile_embed, valid_tiles, offsets, norm_gain, w_qkv, sub_gain, w_out):
    devices = lax.axis_size("seq")
    rows, width = tile_embed.shape
    heads = offsets.shape[0]
    size = width // heads
    pad = size + AUG
    half = devices // 2
    each = rows // devices
    lanes = rows // MIDDLE_DILATION
    few = rows // FAR_DILATION
    scale = float(size) ** -0.5 * LOG2E
    bf16 = lambda *shape: pltpu.VMEM(shape, jnp.bfloat16)
    vmem = pl.BlockSpec(memory_space=pltpu.VMEM)
    smem = pl.BlockSpec(memory_space=pltpu.SMEM)
    anywhere = pl.BlockSpec(memory_space=pl.ANY)
    sems = lambda n: pltpu.SemaphoreType.DMA((n,))
    return pl.pallas_call(
        functools.partial(layer_kernel, heads, devices, scale),
        out_shape=jax.ShapeDtypeStruct((rows, width), jnp.bfloat16),
        in_specs=[smem, smem, anywhere, vmem, anywhere, vmem, anywhere],
        out_specs=vmem,
        scratch_shapes=[
            bf16(2, 2, half, each, width),
            bf16(2, rows, width),
            bf16(*w_qkv.shape),
            bf16(*w_qkv.shape[::-1]),
            bf16(*w_out.shape),
            bf16(3 * heads, pad, 2 * rows),
            pltpu.VMEM((heads, pad, rows), jnp.float32),
            bf16(width, rows),
            bf16(3 * lanes, 4 * lanes),
            pltpu.VMEM((2 * rows, rows), jnp.float32),
            pltpu.VMEM((2 * rows, rows), jnp.float32),
            pltpu.VMEM((1, rows), jnp.float32),
            pltpu.VMEM((1, rows), jnp.float32),
            bf16(heads // 4, 4, size, lanes),
            bf16(heads // 4, 4, size, lanes),
            bf16(heads, pad, 2 * lanes),
            bf16(heads, pad, 2 * lanes),
            pltpu.VMEM((heads, pad, lanes), jnp.float32),
            bf16(heads // 4, 4, pad, lanes),
            bf16(heads // 4, 4, pad, lanes),
            bf16(heads, size, lanes),
            bf16(devices, size, lanes),
            bf16(devices * few, size),
            bf16(devices * few, size),
            bf16(devices * few, size),
            bf16(devices, few, lanes),
            bf16(heads, few, lanes),
            sems(half), sems(half), sems(half), sems(half), sems(half), sems(half),
            sems(heads // 4), sems(heads // 4), sems(heads // 4), sems(heads // 4),
            sems(devices), sems(devices), sems(devices), sems(devices),
            sems(3),
        ],
        compiler_params=pltpu.CompilerParams(
            vmem_limit_bytes=VMEM_LIMIT, collective_id=0, has_side_effects=True
        ),
        name="layer",
    )(
        offsets, valid_tiles, tile_embed.reshape(half, 2, each, width), norm_gain, w_qkv,
        sub_gain, w_out,
    )


def solution(mesh):
    devices = mesh.shape["seq"]

    def body(tile_embed, valid_tiles, offsets, *rest):
        fits = devices == offsets.shape[0] == FAR_DILATION and tile_embed.shape[0] % (16 * devices) == 0
        run = exchanged_body if fits else gathered_body
        return run(tile_embed, valid_tiles, offsets, *rest)

    return jax.shard_map(
        body,
        mesh=mesh,
        in_specs=(P(("slide", "seq"), None), P("slide"), P(), P(), P(), P(), P()),
        out_specs=P(("slide", "seq"), None),
        check_vma=False,
    )
```

```python
import functools

import jax
import jax.numpy as jnp
import numpy as np
from jax import lax
from jax.experimental import pallas as pl
from jax.experimental.pallas import tpu as pltpu
from jax.sharding import PartitionSpec as P

MIDDLE_DILATION = 4
FAR_DILATION = 16
NEGATIVE = -1e30
EPSILON = 1e-05
LOG2E = 1.4426950408889634
AUG = 16
VMEM_LIMIT = 60 * 1024 * 1024


def layer_norm_rows(x, gain):
    average = jnp.mean(x, axis=-1, keepdims=True)
    centred = x - average
    variance = jnp.mean(centred * centred, axis=-1, keepdims=True)
    return centred * lax.rsqrt(variance + EPSILON) * gain


def project_into(dst, x_ref, gain_ref, w_ref, chunk, skip=0):
    normed = layer_norm_rows(x_ref[...].astype(jnp.float32), gain_ref[...]).astype(jnp.bfloat16)

    @pl.loop(0, (w_ref.shape[0] - skip) // chunk)
    def _(i):
        rows = pl.ds(pl.multiple_of(i * chunk, chunk), chunk)
        dst[rows, :] = lax.dot_general(
            w_ref[pl.ds(pl.multiple_of(i * chunk + skip, chunk), chunk), :], normed, (((1,), (1,)), ((), ())), preferred_element_type=jnp.float32
        ).astype(jnp.bfloat16)


def project_kernel(heads, offs, x_ref, gain_ref, w_ref, proj_ref, mid_ref, fark_ref, farv_ref, far_scr):
    rows, width = x_ref.shape
    size = width // heads
    lanes = rows // MIDDLE_DILATION
    few = rows // FAR_DILATION
    project_into(proj_ref, x_ref, gain_ref, w_ref, 256)
    src = lax.broadcasted_iota(jnp.int32, (lanes, lanes), 0)
    dst = lax.broadcasted_iota(jnp.int32, (lanes, lanes), 1)
    for head in range(heads):
        phase = offs[head] % FAR_DILATION
        quarter = phase % MIDDLE_DILATION
        shift = (phase // MIDDLE_DILATION) * few
        pick = ((src == dst + shift) & (dst < few)).astype(jnp.bfloat16)
        for part in range(2):
            base = part * width + head * size
            block = proj_ref[
                width + base : width + base + size,
                pl.ds(pl.multiple_of(quarter * lanes, lanes), lanes),
            ]
            mid_ref[base : base + size, :] = block
            far_scr[base : base + size, :] = jnp.dot(
                block, pick, preferred_element_type=jnp.float32
            )
    fark_ref[...] = far_scr[:width, :].T[:few].astype(jnp.bfloat16)
    farv_ref[...] = far_scr[width:, :].T[:few].astype(jnp.bfloat16)


def aug_rows(first, lanes, second=None):
    spot = lax.broadcasted_iota(jnp.int32, (AUG, lanes), 0)
    rows = jnp.where(spot == 0, first, 0.0)
    if second is not None:
        rows = jnp.where(spot == 1, second, rows)
    return rows.astype(jnp.bfloat16)


def weighted_values(value, weight):
    scaled = (value.astype(jnp.float32) * weight).astype(jnp.bfloat16)
    return jnp.concatenate([scaled, aug_rows(weight, value.shape[1])], axis=0)


def scores_of(keys, queries):
    return lax.dot_general(
        keys, queries, (((0,), (0,)), ((), ())), preferred_element_type=jnp.float32
    )


def own_kernel(scale, per_step, size, valid, q_ref, k_ref, v_ref, pos_ref, out_ref):
    lanes = q_ref.shape[1]
    alive = pos_ref[...] + lax.axis_index("seq") * lanes < valid[0]
    bias = aug_rows(jnp.where(alive, 0.0, NEGATIVE), lanes)
    weight = jnp.where(alive, 1.0, 0.0)
    unit = aug_rows(jnp.ones((1, lanes), jnp.float32), lanes)
    for i in range(per_step):
        part = slice(i * size, (i + 1) * size)
        scores = scores_of(
            jnp.concatenate([k_ref[part, :], bias], axis=0),
            jnp.concatenate([q_ref[part, :], unit], axis=0),
        )
        top = jnp.max(scores, axis=0, keepdims=True)
        p = jnp.exp2((scores - top) * scale).astype(jnp.bfloat16)
        base = i * (size + AUG)
        out_ref[base : base + size + AUG, :] = jnp.dot(
            weighted_values(v_ref[part, :], weight), p, preferred_element_type=jnp.float32
        )
        out_ref[base + size + 1 : base + size + 2, :] = top


def rest_kernel(
    heads, scale, per_step, far_span, middle, offs, valid,
    x_ref, xp_ref, gain_ref, w_ref, q_ref, k_ref, v_ref, own_ref, ppos_ref,
    *rest,
):
    others = middle - 2
    midk, midv = rest[:others], rest[others : 2 * others]
    fark_ref, farv_ref, extra_ref, subgain_ref, wout_ref = rest[2 * others : 2 * others + 5]
    out_ref, kvp, far_t, o_scr, att = rest[2 * others + 5 :]
    rows, width = x_ref.shape
    size = width // heads
    lanes = rows // MIDDLE_DILATION
    few = rows // FAR_DILATION
    step = pl.program_id(0)

    @pl.when(step == 0)
    def _():
        project_into(kvp, xp_ref, gain_ref, w_ref, 256, width)
        for i in range(fark_ref.shape[0] // 128):
            far_t[:width, i * 128 : (i + 1) * 128] = fark_ref[i * 128 : (i + 1) * 128, :].T
            far_t[width:, i * 128 : (i + 1) * 128] = farv_ref[i * 128 : (i + 1) * 128, :].T

    me = lax.axis_index("seq")
    alive = ppos_ref[...] + (me ^ 1) * rows < valid[0]
    bias = aug_rows(jnp.where(alive, 0.0, NEGATIVE), rows)
    weight = jnp.where(alive, 1.0, 0.0)
    unit = aug_rows(jnp.ones((1, rows), jnp.float32), rows)
    is_far = extra_ref[1:2, :]
    device = extra_ref[2:3, :] ^ me
    start = extra_ref[0:1, :] + device * rows
    times = jnp.where((is_far == 1) & (device // far_span == me // far_span), 2, 1)
    lane = lax.broadcasted_iota(jnp.int32, (1, lanes), 1)
    for i in range(per_step):
        head = step * per_step + i
        part = slice(i * size, (i + 1) * size)
        base = i * (size + AUG)
        both = slice(base, base + size + AUG)
        phase = offs[head] % FAR_DILATION
        quarter = phase % MIDDLE_DILATION
        cols = pl.ds(pl.multiple_of(quarter * lanes, lanes), lanes)
        krows = pl.ds(pl.multiple_of(head * size, AUG), size)
        vrows = pl.ds(pl.multiple_of(width + head * size, AUG), size)

        scores = scores_of(
            jnp.concatenate([kvp[krows, :], bias], axis=0),
            jnp.concatenate([q_ref[part, :], unit], axis=0),
        )
        own = own_ref[both, :]
        own_top = own[size + 1 : size + 2, :]
        top = jnp.maximum(own_top, jnp.max(scores, axis=0, keepdims=True))
        p = jnp.exp2((scores - top) * scale).astype(jnp.bfloat16)
        o_scr[both, :] = own * jnp.exp2((own_top - top) * scale) + jnp.dot(
            weighted_values(kvp[vrows, :], weight), p, preferred_element_type=jnp.float32
        )
        o_scr[base + size + 1 : base + size + 2, :] = top

        keys = jnp.concatenate(
            [k_ref[part, cols], kvp[krows, cols]]
            + [midk[g][part, :] for g in range(others)]
            + [far_t[krows, :]],
            axis=1,
        )
        values = jnp.concatenate(
            [v_ref[part, cols], kvp[vrows, cols]]
            + [midv[g][part, :] for g in range(others)]
            + [far_t[vrows, :]],
            axis=1,
        )
        spot = start + jnp.where(is_far == 1, phase, quarter)
        live = spot < valid[0]
        count = jnp.where(live, times, 0).astype(jnp.float32)
        keys = jnp.concatenate(
            [
                keys,
                aug_rows(
                    jnp.where(live, 0.0, NEGATIVE), keys.shape[1], is_far.astype(jnp.float32)
                ),
            ],
            axis=0,
        )
        mine = lane // few == phase // MIDDLE_DILATION
        queries = jnp.concatenate(
            [
                q_ref[part, cols],
                aug_rows(
                    jnp.ones((1, lanes), jnp.float32), lanes, jnp.where(mine, 0.0, NEGATIVE)
                ),
            ],
            axis=0,
        )
        more = scores_of(keys, queries)
        had = o_scr[both, cols]
        had_top = had[size + 1 : size + 2, :]
        new_top = jnp.maximum(had_top, jnp.max(more, axis=0, keepdims=True))
        p = jnp.exp2((more - new_top) * scale).astype(jnp.bfloat16)
        total = had * jnp.exp2((had_top - new_top) * scale) + jnp.dot(
            weighted_values(values, count), p, preferred_element_type=jnp.float32
        )
        o_scr[both, cols] = jnp.where(new_top > 0.5 * NEGATIVE, total, 0.0)
        done = o_scr[both, :]
        result = done[:size] / jnp.maximum(done[size : size + 1], 1.0)
        att[pl.ds(pl.multiple_of(head * size, AUG), size), :] = result.astype(jnp.bfloat16)

    @pl.when(step == pl.num_programs(0) - 1)
    def _():
        attended = att[...].astype(jnp.float32)
        average = jnp.mean(attended, axis=0, keepdims=True)
        centred = attended - average
        variance = jnp.mean(centred * centred, axis=0, keepdims=True)
        normed = centred * lax.rsqrt(variance + EPSILON) * subgain_ref[...]
        projected = jnp.dot(
            normed.T.astype(jnp.bfloat16), wout_ref[...], preferred_element_type=jnp.float32
        )
        out_ref[...] = (x_ref[...].astype(jnp.float32) + projected).astype(jnp.bfloat16)


def doubled(rows, bit, devices):
    pairs = [(d, d ^ (1 << bit)) for d in range(devices)]
    return jnp.concatenate([rows, lax.ppermute(rows, "seq", pairs)], axis=0)


def gathered_body(tile_embed, valid_tiles, offsets, norm_gain, w_qkv, sub_gain, w_out):
    devices = lax.axis_size("seq")
    me = lax.axis_index("seq")
    rows, width = tile_embed.shape
    heads = offsets.shape[0]
    size = width // heads
    lanes = rows // MIDDLE_DILATION
    few = rows // FAR_DILATION
    each = rows // devices
    middle = max(4, devices // 16)
    far_span = max(8, devices // 4)
    per_step = 2
    steps = heads // per_step
    scale = float(size) ** -0.5 * LOG2E

    w_t = w_qkv.T
    pieces = tile_embed.reshape(devices, each, width)
    arrived = lax.all_to_all(pieces, "seq", split_axis=0, concat_axis=0, tiled=True)
    groups = devices // FAR_DILATION
    x = arrived.reshape(groups, 4, 4, each, width).transpose(2, 1, 0, 3, 4).reshape(rows, width)
    xp = lax.ppermute(x, "seq", [(d, d ^ 1) for d in range(devices)])

    whole = lambda *shape: pl.BlockSpec(shape, lambda *_: (0,) * len(shape))
    smem = pl.BlockSpec(memory_space=pltpu.SMEM)
    gain = norm_gain.reshape(1, width)

    proj, mid, far_key, far_value = pl.pallas_call(
        functools.partial(project_kernel, heads),
        out_shape=(
            jax.ShapeDtypeStruct((3 * width, rows), jnp.bfloat16),
            jax.ShapeDtypeStruct((2 * width, lanes), jnp.bfloat16),
            jax.ShapeDtypeStruct((few, width), jnp.bfloat16),
            jax.ShapeDtypeStruct((few, width), jnp.bfloat16),
        ),
        in_specs=[smem] + [pl.BlockSpec(memory_space=pltpu.VMEM)] * 3,
        out_specs=(pl.BlockSpec(memory_space=pltpu.VMEM),) * 4,
        scratch_shapes=[pltpu.VMEM((2 * width, lanes), jnp.float32)],
        compiler_params=pltpu.CompilerParams(vmem_limit_bytes=VMEM_LIMIT),
        cost_estimate=pl.CostEstimate(
            flops=6 * rows * width * width, bytes_accessed=12 * width * width, transcendentals=0
        ),
        name="project",
    )(offsets, x, gain, w_t)

    mids = [
        lax.ppermute(mid, "seq", [(d, d ^ g) for d in range(devices)]) for g in range(2, middle)
    ]
    bits = devices.bit_length() - 1
    for bit in range(bits):
        far_key = doubled(far_key, bit, devices)
        far_value = doubled(far_value, bits - 1 - bit, devices)
    far_value = (
        far_value.reshape((2,) * bits + (few, width))
        .transpose(tuple(reversed(range(bits))) + (bits, bits + 1))
        .reshape(devices * few, width)
    )

    local = np.arange(rows, dtype=np.int32).reshape(each, groups, 4, 4).transpose(3, 2, 1, 0)
    local = local.reshape(1, rows)
    seats = np.arange(devices, dtype=np.int32)
    mid_rows = [np.tile(local[0, :lanes], middle), np.zeros(middle * lanes, np.int32),
                np.repeat(np.arange(middle, dtype=np.int32), lanes)]
    far_rows = [np.tile(local[0, :few], devices), np.ones(devices * few, np.int32),
                np.repeat(seats, few)]
    extra = np.concatenate([np.stack(mid_rows), np.stack(far_rows)], axis=1)
    extra_count = extra.shape[1]

    strip = per_step * size
    out_strip = per_step * (size + AUG)
    block = lambda part: pl.BlockSpec((strip, rows), lambda h: (part * steps + h, 0))
    own = pl.pallas_call(
        functools.partial(own_kernel, scale, per_step, size),
        grid=(steps,),
        out_shape=jax.ShapeDtypeStruct((heads * (size + AUG), rows), jnp.float32),
        in_specs=[smem, block(0), block(1), block(2), whole(1, rows)],
        out_specs=pl.BlockSpec((out_strip, rows), lambda h: (h, 0)),
        compiler_params=pltpu.CompilerParams(vmem_limit_bytes=VMEM_LIMIT),
        cost_estimate=pl.CostEstimate(
            flops=16 * rows * rows * width, bytes_accessed=8 * rows * width,
            transcendentals=heads * rows * rows,
        ),
        name="own_keys",
    )(valid_tiles, proj, proj, proj, jnp.asarray(local))

    out = pl.pallas_call(
        functools.partial(rest_kernel, heads, scale, per_step, far_span, middle),
        grid=(steps,),
        out_shape=jax.ShapeDtypeStruct((rows, width), jnp.bfloat16),
        in_specs=[
            smem, smem,
            whole(rows, width), whole(rows, width), whole(1, width), whole(3 * width, width),
            block(0), block(1), block(2),
            pl.BlockSpec((out_strip, rows), lambda h: (h, 0)),
            whole(1, rows),
            *[pl.BlockSpec((strip, lanes), lambda h: (h, 0))] * len(mids),
            *[pl.BlockSpec((strip, lanes), lambda h: (steps + h, 0))] * len(mids),
            whole(devices * few, width), whole(devices * few, width), whole(3, extra_count),
            whole(width, 1), whole(width, width),
        ],
        out_specs=whole(rows, width),
        scratch_shapes=[
            pltpu.VMEM((2 * width, rows), jnp.bfloat16),
            pltpu.VMEM((2 * width, devices * few), jnp.bfloat16),
            pltpu.VMEM((out_strip, rows), jnp.float32),
            pltpu.VMEM((width, rows), jnp.bfloat16),
        ],
        compiler_params=pltpu.CompilerParams(vmem_limit_bytes=VMEM_LIMIT),
        cost_estimate=pl.CostEstimate(
            flops=24 * rows * rows * width, bytes_accessed=20 * rows * width,
            transcendentals=heads * rows * rows,
        ),
        name="rest",
    )(
        offsets, valid_tiles, x, xp, gain, w_t, proj, proj, proj, own, jnp.asarray(local),
        *mids, *mids, far_key, far_value, jnp.asarray(extra), sub_gain.reshape(width, 1), w_out,
    )
    return (
        out.reshape(4, 4, groups, each, width).transpose(3, 2, 1, 0, 4).reshape(rows, width)
    )


def flip(number, mask):
    for bit in range(mask.bit_length()):
        if mask >> bit & 1:
            number = number + (1 << bit) * (1 - 2 * ((number // (1 << bit)) % 2))
    return number


def to(device):
    return {"seq": device}


def remote(src, dst, send, recv, device):
    return pltpu.make_async_remote_copy(
        src_ref=src, dst_ref=dst, send_sem=send, recv_sem=recv,
        device_id=to(device), device_id_type=pl.DeviceIdType.MESH,
    )


def split_rows(total, top):
    lanes = total.shape[1]
    spot = lax.broadcasted_iota(jnp.int32, (AUG, lanes), 0)
    rounded = lambda a: a.astype(jnp.bfloat16).astype(jnp.float32)
    total_high = rounded(total)
    top_high = rounded(top)
    top_mid = rounded(top - top_high)
    parts = [total_high, total - total_high, top_high, top_mid, top - top_high - top_mid]
    rows = jnp.zeros((AUG, lanes), jnp.float32)
    for i, part in enumerate(parts):
        rows = jnp.where(spot == i, part, rows)
    return rows


def layer_kernel(
    heads, devices, scale,
    offs, valid, x_hbm, gain_ref, w_hbm, subgain_ref, wout_hbm,
    out_ref,
    xr, normed, w_v, w_t, wout_v, qkv, acc, att, bank, s_even, s_odd, t_even, t_odd,
    mq, mqrx, mk, mv, mloc, mres, mret, fmsg, frx, fq, fk, fv, fres, fret,
    s1, r1, s2, r2, s3, r3, ms, mr, ns, nr, fs, fr, gs, gr, ws,
):
    rows, width = out_ref.shape
    size = width // heads
    half = devices // 2
    each = rows // devices
    lanes = rows // MIDDLE_DILATION
    few = rows // FAR_DILATION
    pad = size + AUG
    wide = rows // 2
    batch = 4
    batches = heads // batch
    me = lax.axis_index("seq")
    par = me % 2
    pair = me // 2
    partner = flip(me, 1)
    across = flip(me, 2)

    seat_of = lambda k: (k % 2) * (half // 2) + k // 2
    load_w = pltpu.make_async_copy(w_hbm, w_v, ws.at[0])
    load_w.start()
    load_wout = pltpu.make_async_copy(wout_hbm, wout_v, ws.at[1])
    load_wout.start()
    own_block = pltpu.make_async_copy(x_hbm.at[pair], xr.at[0, :, seat_of(pair)], ws.at[2])
    own_block.start()

    barrier = pltpu.get_barrier_semaphore()
    for d in range(1, devices):
        pl.semaphore_signal(
            barrier, inc=1, device_id=to(flip(me, d)), device_id_type=pl.DeviceIdType.MESH
        )
    pl.semaphore_wait(barrier, devices - 1)

    def first(j):
        other = flip(pair, j)
        return remote(
            x_hbm.at[other], xr.at[0, :, seat_of(pair)], s1.at[j], r1.at[pair], 2 * other + par
        )

    def first_arrival(j):
        other = flip(pair, j)
        return remote(
            x_hbm.at[other], xr.at[0, :, seat_of(other)], s1.at[j], r1.at[other], 2 * other + par
        )

    def forward(j, member, arrives, send, recv):
        k = flip(pair, j)
        return remote(
            xr.at[0, member, seat_of(k)], xr.at[1, arrives, seat_of(k)],
            send.at[j], recv.at[k], partner,
        )

    def urgent(j):
        return forward(j, 1 - par, 1 - par, s2, r2)

    def urgent_arrival(j):
        return forward(j, 1 - par, par, s2, r2)

    def later(j):
        return forward(j, par, par, s3, r3)

    def later_arrival(j):
        return forward(j, par, 1 - par, s3, r3)

    for j in range(1, half):
        first(j).start()
    own_block.wait()
    urgent(0).start()
    later(0).start()

    column = lax.broadcasted_iota(jnp.int32, (1, rows), 1)
    block = column // few
    side = (block // half + par) % 2
    phase = (block % 4) * 4 + ((block % half) // 4) * 2 + side
    place = (column % few) * FAR_DILATION + phase
    unit = aug_rows(jnp.ones((1, rows), jnp.float32), rows)
    alive = [place + device * rows < valid[0] for device in (me, partner)]
    biases = [aug_rows(jnp.where(a, 0.0, NEGATIVE), rows) for a in alive]
    weight_rows = [aug_rows(jnp.where(a, 1.0, 0.0), rows) for a in alive]

    @pl.loop(0, heads)
    def _(h):
        qkv[h, size:, :rows] = unit
        for m in range(2):
            qkv[heads + h, size:, m * rows : (m + 1) * rows] = biases[m]
            qkv[2 * heads + h, size:, m * rows : (m + 1) * rows] = weight_rows[m]

    bank_row = lax.broadcasted_iota(jnp.int32, (3 * lanes, 1), 0)
    bank_col = lax.broadcasted_iota(jnp.int32, (1, batch * lanes), 1)
    spot = bank_col % lanes
    source = jnp.where(
        spot < 3 * few, (spot // few) * lanes + (bank_col // lanes) * few + spot % few, -1
    )
    bank[...] = jnp.where(bank_row == source, 1.0, 0.0).astype(jnp.bfloat16)

    load_w.wait()

    @pl.loop(0, w_v.shape[1] // 256)
    def _(i):
        cols = pl.ds(pl.multiple_of(i * 256, 256), 256)
        w_t[cols, :] = w_v[:, cols].T

    gain = gain_ref[...].reshape(1, width)

    def norm(m, c, first_seat, seats):
        count = seats * each
        piece = xr[c, par + m - 2 * par * m, pl.ds(first_seat, seats)]
        piece = piece.reshape(count, width).astype(jnp.float32)
        at = pl.ds(pl.multiple_of(c * wide + first_seat * each, count), count)
        normed[m, at, :] = layer_norm_rows(piece, gain).astype(jnp.bfloat16)

    quarter_seats = half // 4
    zone = (pair // 2) // quarter_seats
    for g in range(2):
        for j in range(max(1, g * half // 2), (g + 1) * half // 2):
            first_arrival(j).wait_recv()
            urgent(j).start()
            if g == 0:
                later(j).start()
        z = zone if g == 0 else 1 - zone

        @pl.loop(0, 4)
        def _(t):
            norm(t // 2, 0, (t % 2) * (half // 2) + z * quarter_seats, quarter_seats)

    for j in range(half // 2, half):
        later(j).start()

    def project(c, start, stop):
        @pl.loop(start, stop)
        def _(t):
            m = t // 3
            part = t - 2 * m
            at = slice(c * wide, (c + 1) * wide)
            device = me + m * (partner - me)
            weight = jnp.where(place[:, at] + device * rows < valid[0], 1.0, 0.0)
            part_row = jnp.zeros((1, wide), jnp.int32) + part
            factor = jnp.where(part_row == 0, scale, jnp.where(part_row == 2, weight, 1.0))
            result = lax.dot_general(
                w_t[pl.ds(pl.multiple_of(part * width, width), width), :], normed[m, at, :],
                (((1,), (1,)), ((), ())), preferred_element_type=jnp.float32,
            )
            result = (result * factor).astype(jnp.bfloat16)
            where = pl.ds(pl.multiple_of(m * rows + c * wide, wide), wide)
            for i in range(heads):
                qkv[part * heads + i, :size, where] = result[i * size : (i + 1) * size]

    project(0, 0, 3)
    for j in range(half):
        urgent_arrival(j).wait_recv()

    @pl.loop(0, 4)
    def _(t):
        norm(0, 1, t * quarter_seats, quarter_seats)

    project(1, 0, 3)

    def head_turn(h):
        turn = offs[h] % FAR_DILATION
        return turn, ((turn + par) % 2) * 2 + (turn // 2) % 2

    ones = jnp.zeros((1, lanes), jnp.int32)

    def chosen(row, shift, where):
        total = None
        for b in range(MIDDLE_DILATION):
            by = jnp.where(ones + where == b, 1.0, 0.0).astype(jnp.bfloat16)
            piece = qkv[row, :size, shift + b * lanes : shift + (b + 1) * lanes] * by
            total = piece if total is None else total + piece
        return total

    @pl.loop(0, batches)
    def _(c):
        turns = [head_turn(c * batch + i) for i in range(batch)]
        stacked = []
        for i in range(batch):
            h = c * batch + i
            pieces = [chosen(p * heads + h, 0, turns[i][1]) for p in range(3)]
            mq[c, i, :size] = pieces[0]
            mk[h, :size, :lanes] = pieces[1]
            mv[h, :size, :lanes] = pieces[2]
            stacked.append(jnp.concatenate(pieces, axis=1))
        spread = jnp.dot(
            jnp.concatenate(stacked, axis=0), bank[...], preferred_element_type=jnp.float32
        )
        for i in range(batch):
            total = None
            for b in range(4):
                by = jnp.where(ones + turns[i][0] // 4 == b, 1.0, 0.0)
                piece = spread[i * size : (i + 1) * size, b * lanes : (b + 1) * lanes] * by
                total = piece if total is None else total + piece
            fmsg[c * batch + i] = total.astype(jnp.bfloat16)

    def far_send(j):
        other = flip(me, j)
        return remote(fmsg.at[other], frx.at[me], fs.at[j], fr.at[me], other)

    def far_arrival(j):
        other = flip(me, j)
        return remote(fmsg.at[other], frx.at[other], fs.at[j], fr.at[other], other)

    def mid_send(c):
        return remote(mq.at[c], mqrx.at[c], ms.at[c], mr.at[c], across)

    def mid_return(c):
        return remote(mres.at[c], mret.at[c], ns.at[c], nr.at[c], across)

    for j in range(devices - 1, 0, -1):
        far_send(j).start()
    for c in range(batches):
        mid_send(c).start()
    frx[me] = fmsg[me]

    project(0, 3, 5)
    for j in range(half):
        later_arrival(j).wait_recv()

    @pl.loop(0, 4)
    def _(t):
        norm(1, 1, t * quarter_seats, quarter_seats)

    project(1, 3, 5)

    mid_lane = lax.broadcasted_iota(jnp.int32, (1, 2 * lanes), 1)
    mid_place = (
        jnp.where(mid_lane < lanes, me, partner) * rows
        + (mid_lane % few) * FAR_DILATION
        + ((mid_lane % lanes) // few) * MIDDLE_DILATION
    )
    mid_unit = aug_rows(jnp.ones((1, 2 * lanes), jnp.float32), 2 * lanes)

    @pl.loop(0, batches)
    def _(c):
        for i in range(batch):
            h = c * batch + i
            turn, where = head_turn(h)
            mk[h, :size, lanes:] = chosen(heads + h, rows, where)
            mv[h, :size, lanes:] = chosen(2 * heads + h, rows, where)
            live = mid_place + turn % MIDDLE_DILATION < valid[0]
            mk[h, size:, :] = aug_rows(jnp.where(live, 0.0, NEGATIVE), 2 * lanes)
            mv[h, size:, :] = aug_rows(jnp.where(live, 1.0, 0.0), 2 * lanes)

    def far_return(j):
        other = flip(me, j)
        return remote(fres.at[other], fret.at[me], gs.at[j], gr.at[me], other)

    def far_returned(j):
        other = flip(me, j)
        return remote(fres.at[other], fret.at[other], gs.at[j], gr.at[other], other)

    def far_branch():
        for j in range(1, devices):
            far_arrival(j).wait_recv()

        @pl.loop(0, devices // 4)
        def _(g):
            for i in range(4):
                turned = frx[4 * g + i].T
                at = pl.ds(pl.multiple_of((4 * g + i) * few, few), few)
                for p, ref in enumerate((fq, fk, fv)):
                    ref[at, :] = turned[p * few : (p + 1) * few]

        my_turn = offs[me] % FAR_DILATION
        far_size = devices * few // 2
        far_row = lax.broadcasted_iota(jnp.int32, (devices * few, 1), 0)
        far_live = far_row * FAR_DILATION + my_turn < valid[0]
        sums = lax.broadcasted_iota(jnp.int32, (devices * few, AUG), 1) == 0

        @pl.loop(0, 2)
        def _(n):
            scores = lax.dot_general(
                fk[...], fq[pl.ds(pl.multiple_of(n * far_size, far_size), far_size), :],
                (((1,), (1,)), ((), ())), preferred_element_type=jnp.float32,
            )
            scores = jnp.where(far_live, scores, NEGATIVE)
            top = jnp.max(scores, axis=0, keepdims=True)
            p = jnp.exp2(scores - top).astype(jnp.bfloat16)
            count = jnp.where(far_live, jnp.where(far_row // far_size == n, 2.0, 1.0), 0.0)
            numer = lax.dot_general(
                (fv[...].astype(jnp.float32) * count).astype(jnp.bfloat16), p,
                (((0,), (0,)), ((), ())), preferred_element_type=jnp.float32,
            )
            total = lax.dot_general(
                jnp.where(sums, count, 0.0).astype(jnp.bfloat16), p,
                (((0,), (0,)), ((), ())), preferred_element_type=jnp.float32,
            )
            sent = jnp.concatenate(
                [numer, split_rows(total[:1], top),
                 jnp.zeros((lanes - pad, far_size), jnp.float32)], axis=0,
            ).T.astype(jnp.bfloat16)
            for d in range(devices // 2):
                fres[n * (devices // 2) + d] = sent[d * few : (d + 1) * few]

        for j in range(devices - 1, 0, -1):
            far_return(j).start()
        fret[me] = fres[me]

    def middle_scores(c, i):
        queries = jnp.concatenate(
            [jnp.concatenate([mq[c, i], mqrx[c, i]], axis=1), mid_unit], axis=0
        )
        return scores_of(mk[c * batch + i], queries)

    def middle_rest(c, i, scores):
        h = c * batch + i
        top = jnp.max(scores, axis=0, keepdims=True)
        p = jnp.exp2(scores - top).astype(jnp.bfloat16)
        got = jnp.dot(mv[h], p, preferred_element_type=jnp.float32)
        mloc[h] = got[:, :lanes]
        mloc[h, size + 1 : size + 2, :] = top[:, :lanes]
        mres[c, i] = jnp.concatenate(
            [got[:size, lanes:], split_rows(got[size : size + 1, lanes:], top[:, lanes:])],
            axis=0,
        ).astype(jnp.bfloat16)

    key_chunk = rows
    key_chunks = 2 * rows // key_chunk

    def scores_chunk(h, c, dst, best):
        at = slice(c * key_chunk, (c + 1) * key_chunk)
        scores = scores_of(qkv[heads + h, :, at], qkv[h, :, :rows])
        dst[at, :] = scores
        found = jnp.max(scores.reshape(key_chunk // 8, 8, rows), axis=0)
        return found if best is None else jnp.maximum(best, found)

    best = None
    for c in range(key_chunks):
        best = scores_chunk(0, c, s_even, best)
    t_even[...] = jnp.max(best, axis=0, keepdims=True)

    def near_pair(i):
        for u, (now, later_s, top_ref, next_top) in enumerate(
            ((s_even, s_odd, t_even, t_odd), (s_odd, s_even, t_odd, t_even))
        ):
            h = 2 * i + u
            following = 2 * i + 1 if u == 0 else (2 * i + 2) % heads
            top = top_ref[...]
            best = None
            total = None
            for c in range(key_chunks):
                at = slice(c * key_chunk, (c + 1) * key_chunk)
                best = scores_chunk(following, c, later_s, best)
                p = jnp.exp2(now[at, :] - top).astype(jnp.bfloat16)
                part = jnp.dot(qkv[2 * heads + h, :, at], p, preferred_element_type=jnp.float32)
                total = part if total is None else total + part
            acc[h] = total
            acc[h, size + 1 : size + 2, :] = top
            next_top[...] = jnp.max(best, axis=0, keepdims=True)

    before = heads // 4

    @pl.loop(0, before)
    def _(i):
        near_pair(i)

    far_branch()

    @pl.loop(0, batches)
    def _(c):
        mid_send(c).wait_recv()
        for i in range(batch):
            middle_rest(c, i, middle_scores(c, i))
        mid_return(c).start()

    @pl.loop(before, heads // 2)
    def _(i):
        near_pair(i)

    for c in range(batches):
        mid_return(c).wait_recv()
    for j in range(1, devices):
        far_returned(j).wait_recv()

    few_row = lax.broadcasted_iota(jnp.int32, (few, rows), 0)
    even = column % few == few_row

    def stats(a):
        return (
            a[size : size + 1] + a[size + 1 : size + 2],
            a[size + 2 : size + 3] + a[size + 3 : size + 4] + a[size + 4 : size + 5],
        )

    def merge(c, i):
        h = c * batch + i
        turn, _ = head_turn(h)
        in_mid = phase % MIDDLE_DILATION == turn % MIDDLE_DILATION
        in_far = phase == turn
        back = mret[c, i].astype(jnp.float32)
        back_total, back_top = stats(back)
        local_top = mloc[h, size + 1 : size + 2, :]
        mid_top = jnp.maximum(local_top, back_top)
        local_by = jnp.exp2(local_top - mid_top)
        back_by = jnp.exp2(back_top - mid_top)
        mid_total = local_by * mloc[h, size : size + 1, :] + back_by * back_total
        mid_numer = local_by * mloc[h, :size, :] + back_by * back[:size]
        over = lambda a: jnp.concatenate([a] * (rows // lanes), axis=1)
        mid_top = jnp.where(in_mid, over(mid_top), NEGATIVE)
        spread = jnp.where(in_far & even, 1.0, 0.0).astype(jnp.bfloat16)
        far = lax.dot_general(
            fret[h], spread, (((0,), (0,)), ((), ())), preferred_element_type=jnp.float32
        )
        far_total, far_top = stats(far)
        far_top = jnp.where(in_far, far_top, NEGATIVE)
        near_top = acc[h, size + 1 : size + 2, :]
        top = jnp.maximum(near_top, jnp.maximum(mid_top, far_top))
        near_by = jnp.exp2(near_top - top)
        mid_by = jnp.where(in_mid, jnp.exp2(mid_top - top), 0.0)
        far_by = jnp.where(in_far, jnp.exp2(far_top - top), 0.0)
        den = near_by * acc[h, size : size + 1, :] + mid_by * over(mid_total) + far_by * far_total
        inverse = 1.0 / jnp.maximum(den, 1.0)
        numer = (
            (near_by * inverse) * acc[h, :size, :]
            + (mid_by * inverse) * over(mid_numer)
            + (far_by * inverse) * far[:size]
        )
        att[pl.ds(pl.multiple_of(h * size, AUG), size), :] = numer.astype(jnp.bfloat16)

    @pl.loop(0, batches)
    def _(c):
        for i in range(batch):
            merge(c, i)

    load_wout.wait()
    subgain = subgain_ref[...].reshape(1, width)
    @pl.loop(0, 2)
    def _(c):
        target = lax.broadcasted_iota(jnp.int32, (wide, 1), 0) + c * wide
        order = jnp.where(place == target, 1.0, 0.0).astype(jnp.bfloat16)
        attended = lax.dot_general(
            order, att[...], (((1,), (1,)), ((), ())), preferred_element_type=jnp.float32
        )
        residual = jnp.dot(order[:, :wide], xr[0, par].reshape(wide, width), preferred_element_type=jnp.float32)
        residual += jnp.dot(order[:, wide:], xr[1, par].reshape(wide, width), preferred_element_type=jnp.float32)
        sub_normed = layer_norm_rows(attended, subgain).astype(jnp.bfloat16)
        out_ref[pl.ds(pl.multiple_of(c * wide, wide), wide), :] = (
            residual + jnp.dot(sub_normed, wout_v[...], preferred_element_type=jnp.float32)
        ).astype(jnp.bfloat16)

    for j in range(1, half):
        first(j).wait_send()
    for j in range(half):
        urgent(j).wait_send()
        later(j).wait_send()
    for c in range(batches):
        mid_send(c).wait_send()
        mid_return(c).wait_send()
    for j in range(1, devices):
        far_send(j).wait_send()
        far_return(j).wait_send()


def exchanged_body(tile_embed, valid_tiles, offsets, norm_gain, w_qkv, sub_gain, w_out):
    devices = lax.axis_size("seq")
    rows, width = tile_embed.shape
    heads = offsets.shape[0]
    size = width // heads
    pad = size + AUG
    half = devices // 2
    each = rows // devices
    lanes = rows // MIDDLE_DILATION
    few = rows // FAR_DILATION
    scale = float(size) ** -0.5 * LOG2E
    bf16 = lambda *shape: pltpu.VMEM(shape, jnp.bfloat16)
    vmem = pl.BlockSpec(memory_space=pltpu.VMEM)
    smem = pl.BlockSpec(memory_space=pltpu.SMEM)
    anywhere = pl.BlockSpec(memory_space=pl.ANY)
    sems = lambda n: pltpu.SemaphoreType.DMA((n,))
    return pl.pallas_call(
        functools.partial(layer_kernel, heads, devices, scale),
        out_shape=jax.ShapeDtypeStruct((rows, width), jnp.bfloat16),
        in_specs=[smem, smem, anywhere, vmem, anywhere, vmem, anywhere],
        out_specs=vmem,
        scratch_shapes=[
            bf16(2, 2, half, each, width),
            bf16(2, rows, width),
            bf16(*w_qkv.shape),
            bf16(*w_qkv.shape[::-1]),
            bf16(*w_out.shape),
            bf16(3 * heads, pad, 2 * rows),
            pltpu.VMEM((heads, pad, rows), jnp.float32),
            bf16(width, rows),
            bf16(3 * lanes, 4 * lanes),
            pltpu.VMEM((2 * rows, rows), jnp.float32),
            pltpu.VMEM((2 * rows, rows), jnp.float32),
            pltpu.VMEM((1, rows), jnp.float32),
            pltpu.VMEM((1, rows), jnp.float32),
            bf16(heads // 4, 4, size, lanes),
            bf16(heads // 4, 4, size, lanes),
            bf16(heads, pad, 2 * lanes),
            bf16(heads, pad, 2 * lanes),
            pltpu.VMEM((heads, pad, lanes), jnp.float32),
            bf16(heads // 4, 4, pad, lanes),
            bf16(heads // 4, 4, pad, lanes),
            bf16(heads, size, lanes),
            bf16(devices, size, lanes),
            bf16(devices * few, size),
            bf16(devices * few, size),
            bf16(devices * few, size),
            bf16(devices, few, lanes),
            bf16(heads, few, lanes),
            sems(half), sems(half), sems(half), sems(half), sems(half), sems(half),
            sems(heads // 4), sems(heads // 4), sems(heads // 4), sems(heads // 4),
            sems(devices), sems(devices), sems(devices), sems(devices),
            sems(3),
        ],
        compiler_params=pltpu.CompilerParams(
            vmem_limit_bytes=VMEM_LIMIT, collective_id=0, has_side_effects=True
        ),
        name="layer",
    )(
        offsets, valid_tiles, tile_embed.reshape(half, 2, each, width), norm_gain, w_qkv,
        sub_gain, w_out,
    )


def solution(mesh):
    devices = mesh.shape["seq"]

    def body(tile_embed, valid_tiles, offsets, *rest):
        fits = devices == offsets.shape[0] == FAR_DILATION and tile_embed.shape[0] % (16 * devices) == 0
        run = exchanged_body if fits else gathered_body
        return run(tile_embed, valid_tiles, offsets, *rest)

    return jax.shard_map(
        body,
        mesh=mesh,
        in_specs=(P(("slide", "seq"), None), P("slide"), P(), P(), P(), P(), P()),
        out_specs=P(("slide", "seq"), None),
        check_vma=False,
    )
```
